64 devices in a mesh: graphs: 4 (over x, y), nodes: 16 (over z, core).
Axes of the slice: x: 2, y: 2, z: 8, core: 2. Of those that a mesh axis runs over, the one named last changes fastest.
The devices are a block of a 4x4x8 slice.
Arguments:
- x_feat: bfloat16 [32768, 512], P(('graphs', 'nodes')), parts along dimension 0
- valid: int32 [32768], P(('graphs', 'nodes')), parts along dimension 0
- halo_slot: int32 [64, 16, 32], P(('graphs', 'nodes')), parts along dimension 0
- edge_src: int32 [64, 25600], P(('graphs', 'nodes')), parts along dimension 0
- edge_dst: int32 [64, 25600], P(('graphs', 'nodes')), parts along dimension 0
- edge_mask: int32 [64, 25600], P(('graphs', 'nodes')), parts along dimension 0
- bal_perm: int32 [32768], P(('graphs', 'nodes')), parts along dimension 0
- pos_enc: bfloat16 [32768, 512], P(('graphs', 'nodes')), parts along dimension 0
- y_cot: bfloat16 [32768, 512], P(('graphs', 'nodes')), parts along dimension 0
- w_msg: bfloat16 [512, 512], replicated
- w_self: bfloat16 [512, 512], replicated
- w_q: bfloat16 [512, 512], replicated
- w_k: bfloat16 [512, 64], replicated
- w_v: bfloat16 [512, 64], replicated
- w_o: bfloat16 [512, 512], replicated
- w_up: bfloat16 [512, 2048], replicated
- w_down: bfloat16 [2048, 512], replicated
Outputs:
- output 1: bfloat16 [32768, 512], P(('graphs', 'nodes')), parts along dimension 0
- output 2: bfloat16 [32768, 512], P(('graphs', 'nodes')), parts along dimension 0
- output 3: float32 [2048, 512], P('graphs'), parts along dimension 0
- output 4: float32 [2048, 512], P('graphs'), parts along dimension 0
- output 5: float32 [2048, 512], P('graphs'), parts along dimension 0
- output 6: float32 [2048, 64], P('graphs'), parts along dimension 0
- output 7: float32 [2048, 64], P('graphs'), parts along dimension 0
- output 8: float32 [2048, 512], P('graphs'), parts along dimension 0
- output 9: float32 [2048, 2048], P('graphs'), parts along dimension 0
- output 10: float32 [8192, 512], P('graphs'), parts along dimension 0
There are 4 independent parts. The reference program is written for one: setup_inputs(seed, part) draws one part's arguments, and reference() takes and returns one part's arrays. A program takes and returns all parts, laid end to end along the dimension named above; an argument that names none is the same for every part.
All inputs are finite; a program needn't handle non-finite values.
Results may differ from the reference program's by a relative error of at most 0.02.
Values are sent between devices in bfloat16 or wider.
A program may use at most 768 MiB of HBM per device.

```python
import math
import functools
import jax
import jax.numpy as jnp
from jax import lax

NODES = 16
ROWS_DEV = 512
HALO_PAIR = 32
DEG = 50
D = 512
HEADS = 8

HEAD = D // HEADS
HALO = NODES * HALO_PAIR
EDGES = DEG * ROWS_DEV
TOTAL = NODES * ROWS_DEV
QUERY_BLOCK = math.gcd(TOTAL * HEADS, 2 ** max(3, 22 - int(math.log2(TOTAL))))


def draw_perm(key_off, key_rows, key_pos):
    base_count = ROWS_DEV // NODES
    shift_count = base_count // 2
    key_plus, key_gap = jax.random.split(key_off)
    plus_off = jax.random.randint(key_plus, (), 0, NODES)
    minus_off = (plus_off + 1 + jax.random.randint(key_gap, (), 0, NODES - 1)) % NODES
    diagonal = (jnp.arange(NODES)[None, :] - jnp.arange(NODES)[:, None]) % NODES
    counts = base_count + shift_count * (diagonal == plus_off).astype(jnp.int32) - shift_count * (diagonal == minus_off).astype(jnp.int32)
    row_start = jnp.cumsum(counts, axis=1) - counts
    col_end = jnp.cumsum(counts, axis=0)
    col_start = col_end - counts
    row_order = jax.vmap(lambda k: jax.random.permutation(k, ROWS_DEV))(jax.random.split(key_rows, NODES))
    place_ix = jnp.arange(ROWS_DEV)
    owner_ix = jax.vmap(lambda ends: jnp.searchsorted(ends, place_ix, side='right'))(col_end.T)
    dest_ix = jnp.arange(NODES)[:, None]
    offset = place_ix[None, :] - col_start[owner_ix, dest_ix]
    slot_ix = row_order[owner_ix, row_start[owner_ix, dest_ix] + offset]
    global_ix = owner_ix * ROWS_DEV + slot_ix
    shuffle = jax.vmap(lambda k: jax.random.permutation(k, ROWS_DEV))(jax.random.split(key_pos, NODES))
    return jnp.take_along_axis(global_ix, shuffle, axis=1).reshape(TOTAL).astype(jnp.int32)


def draw_layout(key):
    subkeys = jax.random.split(key, 11)
    drop = jax.random.randint(subkeys[0], (NODES,), 0, ROWS_DEV // 32 + 1)
    full_dev = jax.random.randint(subkeys[1], (), 0, NODES)
    n_valid = ROWS_DEV - jnp.where(jnp.arange(NODES) == full_dev, 0, drop)
    valid = (jnp.arange(ROWS_DEV)[None, :] < n_valid[:, None]).astype(jnp.int32).reshape(TOTAL)
    halo_slot = jax.random.randint(subkeys[2], (NODES, NODES, HALO_PAIR), 0, n_valid[None, :, None]).astype(jnp.int32)
    local_src = jax.random.randint(subkeys[3], (NODES, EDGES), 0, n_valid[:, None])
    remote_src = ROWS_DEV + jax.random.randint(subkeys[4], (NODES, EDGES), 0, HALO)
    crosses = jax.random.randint(subkeys[5], (NODES, EDGES), 0, 4) == 0
    edge_src = jnp.where(crosses, remote_src, local_src).astype(jnp.int32)
    edge_dst = jax.random.randint(subkeys[6], (NODES, EDGES), 0, n_valid[:, None]).astype(jnp.int32)
    edge_mask = (jax.random.randint(subkeys[7], (NODES, EDGES), 0, 10) < 9).astype(jnp.int32)
    bal_perm = draw_perm(subkeys[8], subkeys[9], subkeys[10])
    return valid, halo_slot, edge_src, edge_dst, edge_mask, bal_perm


def draw_weight(key, fan_in, fan_out, gain):
    return (jax.random.normal(key, (fan_in, fan_out), jnp.float32) * (gain / math.sqrt(fan_in))).astype(jnp.bfloat16)


def setup_inputs(seed: int = 0, part: int = 0) -> dict:
    root = jax.random.key(seed)
    part_key = jax.random.fold_in(root, part)
    valid, halo_slot, edge_src, edge_dst, edge_mask, bal_perm = draw_layout(jax.random.fold_in(part_key, 1))
    feat_keys = jax.random.split(jax.random.fold_in(part_key, 2), 3)
    weight_keys = jax.random.split(jax.random.fold_in(root, 3), 8)
    score_gain = math.sqrt(0.75 * math.log(TOTAL))
    out_gain = TOTAL ** 0.125
    msg_gain = (0.9 * DEG) ** -0.5
    return {
        'x_feat': jax.random.normal(feat_keys[0], (TOTAL, D), jnp.float32).astype(jnp.bfloat16),
        'valid': valid,
        'halo_slot': halo_slot,
        'edge_src': edge_src,
        'edge_dst': edge_dst,
        'edge_mask': edge_mask,
        'bal_perm': bal_perm,
        'pos_enc': jax.random.normal(feat_keys[1], (TOTAL, D), jnp.float32).astype(jnp.bfloat16),
        'y_cot': jax.random.normal(feat_keys[2], (TOTAL, D), jnp.float32).astype(jnp.bfloat16),
        'w_msg': draw_weight(weight_keys[0], D, D, msg_gain),
        'w_self': draw_weight(weight_keys[1], D, D, 1.0),
        'w_q': draw_weight(weight_keys[2], D, D, score_gain),
        'w_k': draw_weight(weight_keys[3], D, HEAD, 1.0),
        'w_v': draw_weight(weight_keys[4], D, HEAD, 1.0),
        'w_o': draw_weight(weight_keys[5], D, D, out_gain),
        'w_up': draw_weight(weight_keys[6], D, 4 * D, 1.0),
        'w_down': draw_weight(weight_keys[7], 4 * D, D, 1.0),
    }


def to_bf16(a):
    return a.astype(jnp.bfloat16).astype(jnp.float32)


def aggregate(operands):
    table, edge_src, edge_dst, edge_on = operands
    messages = table[edge_src] * edge_on[:, None].astype(jnp.float32)
    return jax.ops.segment_sum(messages, edge_dst, num_segments=ROWS_DEV)


def attend(q_block, keys, values, key_ok):
    scores = jnp.dot(q_block, keys.T, preferred_element_type=jnp.float32) * (HEAD ** -0.5)
    scores = jnp.where(key_ok[None, :], scores, -jnp.inf)
    return jnp.dot(jax.nn.softmax(scores, axis=-1), values, preferred_element_type=jnp.float32)


def layer(x_in, weights, valid, halo_slot, edge_src, edge_dst, edge_mask, bal_perm, pos_enc):
    w_msg, w_self, w_q, w_k, w_v, w_o, w_up, w_down = weights
    owner_base = jnp.arange(NODES)[None, :, None] * ROWS_DEV
    halo_feat = x_in[(halo_slot + owner_base).reshape(NODES, HALO)]
    table = jnp.concatenate([x_in.reshape(NODES, ROWS_DEV, D), halo_feat], axis=1)
    agg_msg = to_bf16(lax.map(aggregate, (table, edge_src, edge_dst, edge_mask)).reshape(TOTAL, D))
    pre_act = jnp.dot(agg_msg, w_msg, preferred_element_type=jnp.float32) + jnp.dot(x_in, w_self, preferred_element_type=jnp.float32)
    hidden_in = to_bf16(x_in[bal_perm] + pos_enc.astype(jnp.float32))
    queries = to_bf16(jnp.dot(hidden_in, w_q, preferred_element_type=jnp.float32)).reshape(TOTAL * HEADS // QUERY_BLOCK, QUERY_BLOCK, HEAD)
    keys = to_bf16(jnp.dot(hidden_in, w_k, preferred_element_type=jnp.float32))
    values = to_bf16(jnp.dot(hidden_in, w_v, preferred_element_type=jnp.float32))
    attend_rows = jax.checkpoint(functools.partial(attend, keys=keys, values=values, key_ok=valid[bal_perm] > 0))
    mixed = to_bf16(lax.map(attend_rows, queries).reshape(TOTAL, D))
    u_bal = to_bf16(jnp.dot(mixed, w_o, preferred_element_type=jnp.float32))
    u_part = jnp.zeros((TOTAL, D), jnp.float32).at[bal_perm].set(u_bal)
    z_mid = to_bf16(x_in + jax.nn.relu(pre_act) + x_in + u_part)
    hidden = to_bf16(jax.nn.gelu(jnp.dot(z_mid, w_up, preferred_element_type=jnp.float32)))
    return jnp.where(valid[:, None] > 0, z_mid + jnp.dot(hidden, w_down, preferred_element_type=jnp.float32), 0.0)


def reference(x_feat, valid, halo_slot, edge_src, edge_dst, edge_mask, bal_perm, pos_enc, y_cot, w_msg, w_self, w_q, w_k, w_v, w_o, w_up, w_down):
    weights = tuple(w.astype(jnp.float32) for w in (w_msg, w_self, w_q, w_k, w_v, w_o, w_up, w_down))
    forward = functools.partial(layer, valid=valid, halo_slot=halo_slot, edge_src=edge_src, edge_dst=edge_dst, edge_mask=edge_mask, bal_perm=bal_perm, pos_enc=pos_enc)
    y_out, pullback = jax.vjp(forward, x_feat.astype(jnp.float32), weights)
    dx_feat, grads = pullback(y_cot.astype(jnp.float32))
    grad_msg, grad_self, grad_q, grad_k, grad_v, grad_o, grad_up, grad_down = grads
    return (y_out.astype(jnp.bfloat16), dx_feat.astype(jnp.bfloat16), grad_msg, grad_self, grad_q, grad_k, grad_v, grad_o, grad_up, grad_down)
```

```python
import functools
import jax
import jax.numpy as jnp
from jax import lax
from jax.experimental import pallas as pl
from jax.experimental.pallas import tpu as pltpu
from jax.sharding import PartitionSpec as P

F32 = jnp.float32
BF16 = jnp.bfloat16
NEG_FILL = -1e30
LANES = 128
MESH = pl.DeviceIdType.MESH


def dot(a, b, ca, cb):
    return lax.dot_general(a, b, (((ca,), (cb,)), ((), ())), preferred_element_type=F32)


def adjacency_kernel(src_ref, dst_ref, out_ref, acc_ref):
    rows, cols = out_ref.shape
    steps, chunk = src_ref.shape
    acc_ref[...] = jnp.zeros_like(acc_ref)
    dst_iota = lax.broadcasted_iota(jnp.int32, (rows, chunk), 0)
    src_iota = lax.broadcasted_iota(jnp.int32, (cols, chunk), 0)

    def body(i, c):
        left = jnp.where(dst_iota == dst_ref[pl.ds(i, 1), :], 1.0, 0.0).astype(BF16)
        right = jnp.where(src_iota == src_ref[pl.ds(i, 1), :], 1.0, 0.0).astype(BF16)
        acc_ref[...] += dot(left, right, 1, 1)
        return c

    lax.fori_loop(0, steps, body, 0)
    out_ref[...] = acc_ref[...].astype(BF16)


def build_adjacency(edge_src, edge_dst, rows, cols, chunk=2560):
    edges = edge_src.size
    if edges % chunk:
        chunk = LANES
    steps = edges // chunk
    return pl.pallas_call(
        adjacency_kernel,
        out_shape=jax.ShapeDtypeStruct((rows, cols), BF16),
        scratch_shapes=[pltpu.VMEM((rows, cols), F32)],
        cost_estimate=pl.CostEstimate(flops=2 * edges * rows * cols, bytes_accessed=2 * rows * cols, transcendentals=0),
        name='adjacency',
    )(edge_src.reshape(steps, chunk), edge_dst.reshape(steps, chunk))


def forward_kernel(k_ref, vt_ref, q_ref, o_ref, lse_ref, *, blocks, group, unroll):
    rows = q_ref.shape[1]
    head_dim = o_ref.shape[0]
    part = vt_ref.shape[2]
    bk = part * group
    q = q_ref[...]

    def body(j, carry):
        run_max, run_sum, acc = carry
        start = pl.multiple_of(j * bk, bk)
        scores = dot(k_ref[pl.ds(start, bk), :], q, 1, 0)
        new_max = jnp.maximum(run_max, jnp.max(scores, axis=0, keepdims=True))
        prob = jnp.exp(scores - new_max)
        decay = jnp.exp(run_max - new_max)
        run_sum = run_sum * decay + jnp.sum(prob, axis=0, keepdims=True)
        prob = prob.astype(BF16)
        acc = acc * decay
        for g in range(group):
            acc = acc + dot(vt_ref[j * group + g, :head_dim, :], prob[g * part:(g + 1) * part], 1, 0)
        return new_max, run_sum, acc

    init = (jnp.full((1, rows), -jnp.inf, F32), jnp.zeros((1, rows), F32), jnp.zeros((head_dim, rows), F32))
    run_max, run_sum, acc = lax.fori_loop(0, blocks, body, init, unroll=unroll)
    o_ref[...] = (acc / run_sum).astype(BF16)
    lse_ref[0] = run_max + jnp.log(run_sum)


def attention_forward(k_ext, vt_ext, qt_ext, heads, head_dim, group=4, unroll=2):
    keys = k_ext.shape[0]
    rows = qt_ext.shape[1]
    nodes, wide, part = vt_ext.shape
    return pl.pallas_call(
        functools.partial(forward_kernel, blocks=nodes // group, group=group, unroll=unroll),
        grid=(heads,),
        in_specs=[
            pl.BlockSpec((keys, LANES), lambda h: (0, 0)),
            pl.BlockSpec((nodes, wide, part), lambda h: (0, 0, 0)),
            pl.BlockSpec((LANES, rows), lambda h: (h, 0)),
        ],
        out_specs=[pl.BlockSpec((head_dim, rows), lambda h: (h, 0)), pl.BlockSpec((1, 1, rows), lambda h: (h, 0, 0))],
        out_shape=[jax.ShapeDtypeStruct((heads * head_dim, rows), BF16), jax.ShapeDtypeStruct((heads, 1, rows), F32)],
        compiler_params=pltpu.CompilerParams(vmem_limit_bytes=56 * 2**20),
        cost_estimate=pl.CostEstimate(flops=4 * heads * rows * keys * head_dim, bytes_accessed=2**23, transcendentals=heads * rows * keys),
        name='attention_forward',
    )(k_ext, vt_ext, qt_ext)


def backward_kernel(kt_ref, vt_ref, q_ref, do_ref, qt_ref, dot_ref, dkv_ref, dq_ref, sums, send_sem, recv_sem, *, nodes, heads, head_dim, unroll):
    bk = kt_ref.shape[-1]
    me = lax.axis_index('nodes')
    right, left = lax.rem(me + 1, nodes), lax.rem(me + nodes - 1, nodes)
    barrier = pltpu.get_barrier_semaphore()
    for neighbour in (left, right):
        pl.semaphore_signal(barrier, inc=1, device_id={'nodes': neighbour}, device_id_type=MESH)
    pl.semaphore_wait(barrier, 2)
    dq_ref[...] = jnp.zeros_like(dq_ref)

    def hop(t):
        return pltpu.make_async_remote_copy(src_ref=sums.at[t], dst_ref=sums.at[t + 1], send_sem=send_sem.at[t], recv_sem=recv_sem.at[t + 1], device_id={'nodes': right}, device_id_type=MESH)

    def step(t, c):
        j = lax.rem(me + 2 * nodes - 1 - t, nodes)
        kt = kt_ref[j]
        vt = vt_ref[j]
        k_top = kt[:head_dim]

        def body(h, carry):
            dk, dv = carry
            lo = pl.multiple_of(h * LANES, LANES)
            r0 = pl.multiple_of(h * head_dim, head_dim)
            prob = jnp.exp(dot(q_ref[:, pl.ds(lo, LANES)], kt, 1, 0))
            d_prob = dot(do_ref[:, pl.ds(lo, LANES)], vt, 1, 0)
            d_scores = (prob * d_prob).astype(BF16)
            dv = dv + dot(dot_ref[pl.ds(r0, head_dim), :], prob.astype(BF16), 1, 0)
            dk = dk + dot(qt_ref[pl.ds(lo, head_dim), :], d_scores, 1, 0)
            dq_ref[pl.ds(r0, head_dim), :] += dot(k_top, d_scores, 1, 1)
            return dk, dv

        zero = jnp.zeros((head_dim, bk), F32)
        dk, dv = lax.fori_loop(0, heads, body, (zero, zero), unroll=unroll)

        @pl.when(t == 0)
        def _():
            sums[t, :head_dim, :] = dk
            sums[t, head_dim:, :] = dv

        @pl.when(t > 0)
        def _():
            hop(t - 1).wait_recv()
            sums[t, :head_dim, :] += dk
            sums[t, head_dim:, :] += dv

        @pl.when(t < nodes - 1)
        def _():
            hop(t).start()
        return c

    lax.fori_loop(0, nodes, step, 0)

    def finish(t, c):
        hop(t).wait_send()
        return c

    lax.fori_loop(0, nodes - 1, finish, 0)
    dkv_ref[...] = sums[nodes - 1].astype(BF16)


def attention_backward(kt_ext, vt_ext, q_ext, do_ext, qt_ext, do_t, heads, head_dim, unroll=4):
    nodes, wide, bk = kt_ext.shape
    rows = q_ext.shape[0]
    return pl.pallas_call(
        functools.partial(backward_kernel, nodes=nodes, heads=heads, head_dim=head_dim, unroll=unroll),
        in_specs=[pl.BlockSpec(memory_space=pltpu.VMEM)] * 6,
        out_specs=[pl.BlockSpec(memory_space=pltpu.VMEM)] * 2,
        out_shape=[jax.ShapeDtypeStruct((2 * head_dim, bk), BF16), jax.ShapeDtypeStruct((heads * head_dim, rows), F32)],
        scratch_shapes=[pltpu.VMEM((nodes, 2 * head_dim, bk), F32), pltpu.SemaphoreType.DMA((nodes,)), pltpu.SemaphoreType.DMA((nodes,))],
        compiler_params=pltpu.CompilerParams(vmem_limit_bytes=40 * 2**20, collective_id=0, has_side_effects=True),
        cost_estimate=pl.CostEstimate(flops=10 * heads * rows * nodes * bk * head_dim, bytes_accessed=2**24, transcendentals=heads * rows * nodes * bk),
        name='attention_backward',
    )(kt_ext, vt_ext, q_ext, do_ext, qt_ext, do_t)


def reduce_kernel(x_ref, out_ref, half, parts, pair_send, pair_recv, part_send, part_recv, full_send, full_recv, back_send, back_recv, *, nodes):
    me = lax.axis_index('nodes')
    chips = nodes // 2
    core = lax.rem(me, 2)
    chip = me // 2
    partner = me + 1 - 2 * core
    rows = x_ref.shape[0]
    hr = rows // 2
    pr = hr // chips
    mine = pl.multiple_of(core * hr, hr)
    other = pl.multiple_of((1 - core) * hr, hr)

    def peer(k):
        return lax.rem(chip + k, chips)

    barrier = pltpu.get_barrier_semaphore()
    pl.semaphore_signal(barrier, inc=1, device_id={'nodes': partner}, device_id_type=MESH)
    for k in range(1, chips):
        pl.semaphore_signal(barrier, inc=1, device_id={'nodes': 2 * peer(k) + core}, device_id_type=MESH)
    pl.semaphore_wait(barrier, chips)

    swap = pltpu.make_async_remote_copy(src_ref=x_ref.at[pl.ds(other, hr)], dst_ref=half, send_sem=pair_send, recv_sem=pair_recv, device_id={'nodes': partner}, device_id_type=MESH)
    swap.start()
    swap.wait_recv()
    half[...] += x_ref[pl.ds(mine, hr)]

    def scatter(k):
        to = peer(k)
        return pltpu.make_async_remote_copy(src_ref=half.at[pl.ds(pl.multiple_of(to * pr, pr), pr)], dst_ref=parts.at[k], send_sem=part_send.at[k], recv_sem=part_recv.at[k], device_id={'nodes': 2 * to + core}, device_id_type=MESH)

    for k in range(1, chips):
        scatter(k).start()
    total = half[pl.ds(pl.multiple_of(chip * pr, pr), pr)]
    for k in range(1, chips):
        scatter(k).wait_recv()
        total = total + parts[k]
    own = pl.multiple_of(core * hr + chip * pr, pr)
    out_ref[pl.ds(own, pr)] = total

    def spread(k):
        return pltpu.make_async_remote_copy(src_ref=out_ref.at[pl.ds(own, pr)], dst_ref=out_ref.at[pl.ds(own, pr)], send_sem=full_send.at[k], recv_sem=full_recv.at[k], device_id={'nodes': 2 * peer(k) + core}, device_id_type=MESH)

    def back(k):
        at = pl.multiple_of(core * hr + lax.rem(chip + chips - k, chips) * pr, pr)
        return pltpu.make_async_remote_copy(src_ref=out_ref.at[pl.ds(at, pr)], dst_ref=out_ref.at[pl.ds(at, pr)], send_sem=back_send.at[k], recv_sem=back_recv.at[k], device_id={'nodes': partner}, device_id_type=MESH)

    for k in range(1, chips):
        spread(k).start()
    back(0).start()
    for k in range(1, chips):
        spread(k).wait_recv()
        back(k).start()
    for k in range(chips):
        back(k).wait_recv()
    swap.wait_send()
    for k in range(1, chips):
        scatter(k).wait_send()
        spread(k).wait_send()
    for k in range(chips):
        back(k).wait_send()


def reduce_all(x, nodes):
    rows, cols = x.shape
    chips = nodes // 2
    pr = rows // nodes
    sems = lambda: pltpu.SemaphoreType.DMA((chips,))
    return pl.pallas_call(
        functools.partial(reduce_kernel, nodes=nodes),
        in_specs=[pl.BlockSpec(memory_space=pltpu.VMEM)],
        out_specs=pl.BlockSpec(memory_space=pltpu.VMEM),
        out_shape=jax.ShapeDtypeStruct(x.shape, F32),
        scratch_shapes=[pltpu.VMEM((rows // 2, cols), F32), pltpu.VMEM((chips, pr, cols), F32), pltpu.SemaphoreType.DMA, pltpu.SemaphoreType.DMA, sems(), sems(), sems(), sems(), sems(), sems()],
        compiler_params=pltpu.CompilerParams(vmem_limit_bytes=16 * 2**20, collective_id=1, has_side_effects=True),
        cost_estimate=pl.CostEstimate(flops=10**10, bytes_accessed=2**23, transcendentals=0),
        name='reduce_all',
    )(x)


def one_hot(index, size):
    return (lax.broadcasted_iota(jnp.int32, (size, index.size), 0) == index[None, :]).astype(BF16)


def exchange(rows, send_ix, recv_ix, nodes):
    count, width = rows.shape
    capacity = count // nodes + count // (2 * nodes)
    picked = dot(one_hot(send_ix, nodes * capacity), rows, 1, 0).astype(BF16)
    landed = lax.all_to_all(picked.reshape(nodes, capacity, width), 'nodes', 0, 0, tiled=True)
    return dot(one_hot(recv_ix, nodes * capacity), landed.reshape(nodes * capacity, width), 0, 0).astype(BF16)


def routes(bal_perm, bal_all, rows_dev, nodes):
    capacity = rows_dev // nodes + rows_dev // (2 * nodes)
    before = (lax.broadcasted_iota(jnp.int32, (rows_dev, rows_dev), 0) < lax.broadcasted_iota(jnp.int32, (rows_dev, rows_dev), 1))
    owner = bal_perm // rows_dev
    same = owner[:, None] == owner[None, :]
    bal_ix = owner * capacity + jnp.sum((same & before).astype(jnp.int32), axis=0)
    me = lax.axis_index('nodes')
    mine = (bal_all // rows_dev == me).astype(BF16)
    rank = dot(mine, before.astype(BF16), 1, 0).astype(jnp.int32)
    code = lax.broadcasted_iota(jnp.int32, rank.shape, 0) * capacity + rank
    wanted = me * rows_dev + jnp.arange(rows_dev, dtype=jnp.int32)
    hit = bal_all.reshape(-1)[:, None] == wanted[None, :]
    part_ix = jnp.sum(jnp.where(hit, code.reshape(-1)[:, None], 0), axis=0)
    return bal_ix, part_ix


def split3(x):
    keep = lambda a: lax.reduce_precision(a, 8, 7)
    hi = keep(x)
    mid = keep(x - hi)
    return jnp.concatenate([hi, mid, keep(x - hi - mid)], axis=0).astype(BF16)


def pad_heads(w, heads, axis):
    if axis == 1:
        w3 = w.reshape(w.shape[0], heads, -1)
        return jnp.pad(w3, ((0, 0), (0, 0), (0, LANES - w3.shape[2]))).reshape(w.shape[0], heads * LANES)
    w3 = w.reshape(heads, -1, w.shape[1])
    return jnp.pad(w3, ((0, 0), (0, LANES - w3.shape[1]), (0, 0))).reshape(heads * LANES, w.shape[1])


def extra_columns(parts, heads, first):
    r = lax.broadcasted_iota(jnp.int32, (3 * heads, heads * LANES), 0)
    c = lax.broadcasted_iota(jnp.int32, (3 * heads, heads * LANES), 1)
    place = (r % heads == c // LANES) & (c % LANES == first + r // heads)
    return dot(parts, place.astype(BF16), 0, 0)


def solution(mesh):
    nodes = mesh.shape['nodes']
    row_spec = P(('graphs', 'nodes'), None)
    flat_spec = P(('graphs', 'nodes'))
    halo_spec = P(('graphs', 'nodes'), None, None)
    grad_spec = P('graphs', None)

    def device_step(x_feat, valid, halo_slot, edge_src, edge_dst, edge_mask, bal_perm, pos_enc, y_cot, w_msg, w_self, w_q, w_k, w_v, w_o, w_up, w_down):
        rows_dev, width = x_feat.shape
        head_dim = w_k.shape[1]
        heads = width // head_dim
        scale = head_dim ** -0.5
        me = lax.axis_index('nodes')
        halo_req = halo_slot.reshape(-1)
        halo_rows = halo_req.size

        count = jnp.sum((valid > 0).astype(jnp.int32))
        info = lax.all_gather(jnp.concatenate([bal_perm, halo_req, jnp.broadcast_to(count, (LANES,))]), 'nodes')
        bal_all = info[:, :rows_dev]
        halo_all = info[:, rows_dev:rows_dev + halo_rows].reshape(nodes, nodes, -1)
        count_all = info[:, rows_dev + halo_rows]
        bal_ix, part_ix = routes(bal_perm, bal_all, rows_dev, nodes)
        owner_all = bal_all // rows_dev
        limit = jnp.sum(jnp.where(owner_all[:, :, None] == jnp.arange(nodes, dtype=jnp.int32), count_all[None, None, :], 0), axis=2)
        key_bias = jnp.where(bal_all % rows_dev < limit, 0.0, NEG_FILL).astype(BF16)

        x_bal = exchange(x_feat, part_ix, bal_ix, nodes)
        hidden_in = (x_bal.astype(F32) + pos_enc.astype(F32)).astype(BF16)
        w_kv = jnp.concatenate([w_k, w_v], axis=1)
        kv_t = dot(w_kv, hidden_in, 0, 1).astype(BF16)
        kv_all = lax.all_gather(kv_t, 'nodes')
        wq_pad = pad_heads((w_q.astype(F32) * scale).astype(BF16), heads, 1)
        row_one = (lax.broadcasted_iota(jnp.int32, (heads * LANES, 1), 0) % LANES == head_dim).astype(F32)
        qt_ext = (dot(wq_pad, hidden_in, 0, 1) + row_one).astype(BF16)

        halo_got = lax.dynamic_index_in_dim(halo_all, me, axis=1, keepdims=False).reshape(-1)
        halo_pick = one_hot(halo_got, rows_dev)
        halo_send = dot(halo_pick, x_feat, 0, 0).astype(BF16)
        halo_feat = lax.all_to_all(halo_send.reshape(nodes, -1, width), 'nodes', 0, 0, tiled=True).reshape(halo_rows, width)
        live_dst = jnp.where(edge_mask.reshape(-1) > 0, edge_dst.reshape(-1), -1)
        adjacency = build_adjacency(edge_src.reshape(-1), live_dst, rows_dev, rows_dev + halo_rows)
        adj_own, adj_halo = adjacency[:, :rows_dev], adjacency[:, rows_dev:]
        agg_msg = (dot(adj_own, x_feat, 1, 0) + dot(adj_halo, halo_feat, 1, 0)).astype(BF16)
        pre_act = dot(agg_msg, w_msg, 1, 0) + dot(x_feat, w_self, 1, 0)

        wide = lambda n: (nodes, n, rows_dev)
        ones3 = jnp.ones(wide(3), BF16)
        kt_ext = jnp.concatenate([kv_all[:, :head_dim], key_bias[:, None, :], ones3, jnp.zeros(wide(LANES - head_dim - 4), BF16)], axis=1)
        vt_ext = jnp.concatenate([kv_all[:, head_dim:], ones3, jnp.zeros(wide(LANES - head_dim - 3), BF16)], axis=1)
        k_ext = kt_ext.transpose(0, 2, 1).reshape(nodes * rows_dev, LANES)
        mixed_t, log_norm = attention_forward(k_ext, vt_ext, qt_ext, heads, head_dim)
        u_bal = dot(mixed_t, w_o, 0, 0).astype(BF16)
        u_part = exchange(u_bal, bal_ix, part_ix, nodes)

        x_wide = x_feat.astype(F32)
        z_mid = (x_wide + jax.nn.relu(pre_act) + x_wide + u_part.astype(F32)).astype(BF16)
        h_pre = dot(z_mid, w_up, 1, 0)
        hidden = jax.nn.gelu(h_pre).astype(BF16)
        keep_row = valid[:, None] > 0
        y_out = jnp.where(keep_row, z_mid.astype(F32) + dot(hidden, w_down, 1, 0), 0.0).astype(BF16)

        g_out = jnp.where(keep_row, y_cot, jnp.zeros_like(y_cot))
        d_hidden = dot(g_out, w_down, 1, 1).astype(BF16)
        gelu_pull = jax.vjp(jax.nn.gelu, h_pre)[1]
        d_hpre = gelu_pull(d_hidden.astype(F32))[0].astype(BF16)
        d_z = (g_out.astype(F32) + dot(d_hpre, w_up, 1, 1)).astype(BF16)
        d_u = exchange(d_z, part_ix, bal_ix, nodes)

        grad_down = dot(hidden, g_out, 0, 0)
        grad_up = dot(z_mid, d_hpre, 0, 0)
        d_pre = jnp.where(pre_act > 0, d_z, jnp.zeros_like(d_z))
        grad_self = dot(x_feat, d_pre, 0, 0)
        grad_msg = dot(agg_msg, d_pre, 0, 0)
        grad_o = dot(mixed_t, d_u, 1, 0)
        grad_msg, grad_self, grad_o, grad_up, grad_down = lax.psum((grad_msg, grad_self, grad_o, grad_up, grad_down), 'nodes')

        do_t = dot(w_o, d_u, 1, 1).astype(BF16)
        delta = jnp.sum((do_t.astype(F32) * mixed_t.astype(F32)).reshape(heads, head_dim, rows_dev), axis=1)
        do_ext = (dot(d_u, pad_heads(w_o, heads, 0), 1, 1) + extra_columns(split3(-delta), heads, head_dim)).astype(BF16)
        col_one = (lax.broadcasted_iota(jnp.int32, (1, heads * LANES), 1) % LANES == head_dim).astype(F32)
        q_ext = (dot(hidden_in, wq_pad, 1, 0) + col_one + extra_columns(split3(-log_norm.reshape(heads, rows_dev)), heads, head_dim + 1)).astype(BF16)
        dkv_t, dq_t = attention_backward(kt_ext, vt_ext, q_ext, do_ext, qt_ext, do_t, heads, head_dim)
        dq_t = (dq_t * scale).astype(BF16)

        d_agg = dot(d_pre, w_msg, 1, 1).astype(BF16)
        d_halo = dot(adj_halo, d_agg, 0, 0).astype(BF16)
        halo_landed = lax.all_to_all(d_halo.reshape(nodes, -1, width), 'nodes', 0, 0, tiled=True).reshape(halo_rows, width)
        local_part = 2.0 * d_z.astype(F32) + dot(d_pre, w_self, 1, 1) + dot(adj_own, d_agg, 0, 0) + dot(halo_pick, halo_landed, 1, 0)

        grad_q = dot(hidden_in, dq_t, 0, 1)
        grad_kv = dot(hidden_in, dkv_t, 0, 1)
        dx_bal = dot(jnp.concatenate([dq_t, dkv_t], axis=0), jnp.concatenate([w_q, w_kv], axis=1), 0, 1).astype(BF16)
        attn_back = exchange(dx_bal, bal_ix, part_ix, nodes)
        dx_feat = (local_part + attn_back.astype(F32)).astype(BF16)
        late = reduce_all(jnp.concatenate([grad_q, grad_kv], axis=1), nodes)
        grad_q, grad_k, grad_v = late[:, :width], late[:, width:width + head_dim], late[:, width + head_dim:]
        return y_out, dx_feat, grad_msg, grad_self, grad_q, grad_k, grad_v, grad_o, grad_up, grad_down

    return jax.shard_map(device_step, mesh=mesh, in_specs=(row_spec, flat_spec, halo_spec, row_spec, row_spec, row_spec, flat_spec, row_spec, row_spec) + (P(),) * 8, out_specs=(row_spec, row_spec) + (grad_spec,) * 8, check_vma=False)
```

```python
import functools
import jax
import jax.numpy as jnp
from jax import lax
from jax.experimental import pallas as pl
from jax.experimental.pallas import tpu as pltpu
from jax.sharding import PartitionSpec as P

F32 = jnp.float32
BF16 = jnp.bfloat16
NEG_FILL = -1e30
LANES = 128
MESH = pl.DeviceIdType.MESH


def dot(a, b, ca, cb):
    return lax.dot_general(a, b, (((ca,), (cb,)), ((), ())), preferred_element_type=F32)


def entry_kernel(x_ref, info_ref, halo_ref, src_ref, dst_ref, x_bal_ref, adj_ref, bal_ix_ref, part_ix_ref, info_all, halo_got, acc_ref, own_ref, rank_ref, send_buf, recv_buf, info_send, info_recv, halo_send, halo_recv, row_send, row_recv, *, nodes):
    me = lax.axis_index('nodes')
    rows = x_ref.shape[0]
    cols = adj_ref.shape[1]
    steps, chunk = src_ref.shape
    capacity = send_buf.shape[1]
    peer = lambda k: lax.rem(me + k, nodes)
    barrier = pltpu.get_barrier_semaphore()

    def greet(k, c):
        pl.semaphore_signal(barrier, inc=1, device_id={'nodes': peer(k)}, device_id_type=MESH)
        return c

    lax.fori_loop(1, nodes, greet, 0)
    acc_ref[...] = jnp.zeros_like(acc_ref)
    dst_iota = lax.broadcasted_iota(jnp.int32, (rows, chunk), 0)
    src_iota = lax.broadcasted_iota(jnp.int32, (cols, chunk), 0)

    def count(i, c):
        left = jnp.where(dst_iota == dst_ref[pl.ds(i, 1), :], 1.0, 0.0).astype(BF16)
        right = jnp.where(src_iota == src_ref[pl.ds(i, 1), :], 1.0, 0.0).astype(BF16)
        acc_ref[...] += dot(left, right, 1, 1)
        return c

    first, second = steps // 10, steps // 2
    lax.fori_loop(0, first, count, 0)
    pl.semaphore_wait(barrier, nodes - 1)

    def tell(k):
        return pltpu.make_async_remote_copy(src_ref=info_ref.at[0], dst_ref=info_all.at[me], send_sem=info_send.at[k], recv_sem=info_recv.at[k], device_id={'nodes': peer(k)}, device_id_type=MESH)

    def ask(k):
        return pltpu.make_async_remote_copy(src_ref=halo_ref.at[peer(k)], dst_ref=halo_got.at[me], send_sem=halo_send.at[k], recv_sem=halo_recv.at[k], device_id={'nodes': peer(k)}, device_id_type=MESH)

    def give(k):
        return pltpu.make_async_remote_copy(src_ref=send_buf.at[k], dst_ref=recv_buf.at[me], send_sem=row_send.at[k], recv_sem=row_recv.at[k], device_id={'nodes': peer(k)}, device_id_type=MESH)

    def start_info(k, c):
        tell(k).start()
        ask(k).start()
        return c

    lax.fori_loop(1, nodes, start_info, 0)
    info_all[me] = info_ref[0]
    halo_got[me] = halo_ref[me]
    lax.fori_loop(first, second, count, 0)

    def wait_info(k, c):
        tell(k).wait_recv()
        return c

    lax.fori_loop(1, nodes, wait_info, 0)

    def mark(q, c):
        own_ref[pl.ds(q, 1), :] = jnp.where(lax.div(info_all[q][:, :rows], rows) == me, 1.0, 0.0)
        return c

    lax.fori_loop(0, nodes, mark, 0)
    before = jnp.where(lax.broadcasted_iota(jnp.int32, (rows, rows), 0) < lax.broadcasted_iota(jnp.int32, (rows, rows), 1), 1.0, 0.0).astype(BF16)
    rank_ref[...] = dot(own_ref[...].astype(BF16), before, 1, 0)
    slot_iota = lax.broadcasted_iota(jnp.int32, (rows, rows), 0)
    cap_iota = lax.broadcasted_iota(jnp.int32, (capacity, rows), 0)
    x = x_ref[...]

    def pick_rows(k, part_ix):
        q = peer(k)
        perm = info_all[q][:, :rows]
        own = lax.div(perm, rows) == me
        rank = jnp.where(own, rank_ref[pl.ds(q, 1), :].astype(jnp.int32), -1)
        ranked = jnp.where(cap_iota == rank, 1.0, 0.0).astype(BF16)
        placed = jnp.where(slot_iota == lax.rem(perm, rows), 1.0, 0.0).astype(BF16)
        pick = dot(ranked, placed, 1, 1)
        send_buf[k] = dot(pick.astype(BF16), x, 1, 0).astype(BF16)

        @pl.when(k > 0)
        def _():
            give(k).start()

        code = (cap_iota + q * capacity).astype(F32)
        return part_ix + jnp.sum(pick * code, axis=0, keepdims=True)

    part_ix = lax.fori_loop(0, nodes, pick_rows, jnp.zeros((1, rows), F32))
    part_ix_ref[...] = part_ix.astype(jnp.int32)
    recv_buf[me] = send_buf[0]
    lax.fori_loop(second, steps, count, 0)
    adj_ref[...] = acc_ref[...].astype(BF16)

    owner = lax.div(info_ref[0][:, :rows], rows)
    owners = lax.broadcasted_iota(jnp.int32, (nodes, rows), 0) == owner
    ranks = dot(jnp.where(owners, 1.0, 0.0).astype(BF16), before, 1, 0)
    bal_ix = owner * capacity + jnp.sum(jnp.where(owners, ranks, 0.0), axis=0, keepdims=True).astype(jnp.int32)
    bal_ix_ref[...] = bal_ix

    def wait_rows(k, c):
        give(k).wait_recv()
        ask(k).wait_recv()
        return c

    lax.fori_loop(1, nodes, wait_rows, 0)
    landed = jnp.where(lax.broadcasted_iota(jnp.int32, (nodes * capacity, rows), 0) == bal_ix, 1.0, 0.0).astype(BF16)
    x_bal_ref[...] = dot(landed, recv_buf[...].reshape(nodes * capacity, x.shape[1]), 0, 0).astype(BF16)

    def wait_sends(k, c):
        tell(k).wait_send()
        ask(k).wait_send()
        give(k).wait_send()
        return c

    lax.fori_loop(1, nodes, wait_sends, 0)


def entry(x, info, halo, edge_src, edge_dst, nodes, chunk=2560):
    rows, width = x.shape
    edges = edge_src.size
    if edges % chunk:
        chunk = LANES
    steps = edges // chunk
    capacity = rows // nodes + rows // (2 * nodes)
    cols = 2 * rows
    i32 = jnp.int32
    sems = lambda: pltpu.SemaphoreType.DMA((nodes,))
    return pl.pallas_call(
        functools.partial(entry_kernel, nodes=nodes),
        in_specs=[pl.BlockSpec(memory_space=pltpu.VMEM)] * 5,
        out_specs=[pl.BlockSpec(memory_space=pltpu.VMEM)] * 6,
        out_shape=[
            jax.ShapeDtypeStruct((rows, width), BF16),
            jax.ShapeDtypeStruct((rows, cols), BF16),
            jax.ShapeDtypeStruct((1, rows), i32),
            jax.ShapeDtypeStruct((1, rows), i32),
            jax.ShapeDtypeStruct((nodes,) + info.shape[1:], i32),
            jax.ShapeDtypeStruct(halo.shape, i32),
        ],
        scratch_shapes=[
            pltpu.VMEM((rows, cols), F32),
            pltpu.VMEM((nodes, rows), F32),
            pltpu.VMEM((nodes, rows), F32),
            pltpu.VMEM((nodes, capacity, width), BF16),
            pltpu.VMEM((nodes, capacity, width), BF16),
            sems(), sems(), sems(), sems(), sems(), sems(),
        ],
        compiler_params=pltpu.CompilerParams(vmem_limit_bytes=40 * 2**20, collective_id=2, has_side_effects=True),
        cost_estimate=pl.CostEstimate(flops=2 * edges * rows * cols, bytes_accessed=2**22, transcendentals=0),
        name='entry',
    )(x, info, halo, edge_src.reshape(steps, chunk), edge_dst.reshape(steps, chunk))


def forward_kernel(kv_ref, bias_ref, q_ref, o_ref, lse_ref, kt_ref, vt_ref, kv_all, k_pair, max_ref, sum_ref, acc_ref, to_right, from_left, to_left, from_right, *, nodes, heads, head_dim, unroll):
    me = lax.axis_index('nodes')
    part = kv_ref.shape[1]
    rows = q_ref.shape[1]
    half = nodes // 2
    right, left = lax.rem(me + 1, nodes), lax.rem(me + nodes - 1, nodes)
    barrier = pltpu.get_barrier_semaphore()
    for neighbour in (left, right):
        pl.semaphore_signal(barrier, inc=1, device_id={'nodes': neighbour}, device_id_type=MESH)
    pl.semaphore_wait(barrier, 2)

    def hop(src, j, t, send, recv, to):
        return pltpu.make_async_remote_copy(src_ref=src, dst_ref=kv_all.at[j], send_sem=send.at[t], recv_sem=recv.at[t], device_id={'nodes': to}, device_id_type=MESH)

    hop(kv_ref, me, 0, to_left, from_right, left).start()
    hop(kv_ref, me, 0, to_right, from_left, right).start()
    kv_all[me] = kv_ref[...]
    max_ref[...] = jnp.full(max_ref.shape, -jnp.inf, F32)
    sum_ref[...] = jnp.zeros_like(sum_ref)
    acc_ref[...] = jnp.zeros_like(acc_ref)
    row_iota = lax.broadcasted_iota(jnp.int32, (head_dim, part), 0)
    v_extra = jnp.where(row_iota < 3, 1.0, 0.0).astype(BF16)

    def widen(j, g):
        block = kv_all[j]
        k_extra = jnp.where(row_iota == 0, bias_ref[j], jnp.where(row_iota < 4, 1.0, 0.0)).astype(BF16)
        wide = jnp.concatenate([block[:head_dim], k_extra], axis=0)
        kt_ref[j] = wide
        vt_ref[j, :head_dim, :] = block[head_dim:]
        vt_ref[j, head_dim:, :] = v_extra
        k_pair[g * part:(g + 1) * part, :] = wide.T

    def step(t, c):
        jr = lax.rem(me + 1 + t, nodes)
        jl = lax.rem(me + nodes - t, nodes)
        hop(kv_all.at[jr], jr, t, to_left, from_right, left).wait_recv()

        @pl.when(t < half - 1)
        def _():
            hop(kv_all.at[jr], jr, t + 1, to_left, from_right, left).start()

        @pl.when(t > 0)
        def _():
            hop(kv_all.at[jl], jl, t - 1, to_right, from_left, right).wait_recv()

        @pl.when((t > 0) & (t < half - 1))
        def _():
            hop(kv_all.at[jl], jl, t, to_right, from_left, right).start()

        widen(jl, 0)
        widen(jr, 1)
        vl = kv_all[jl, head_dim:, :]
        vr = kv_all[jr, head_dim:, :]

        def body(h, c):
            lo = pl.multiple_of(h * LANES, LANES)
            r0 = pl.multiple_of(h * head_dim, head_dim)
            scores = dot(k_pair[...], q_ref[pl.ds(lo, LANES), :], 1, 0)
            old_max = max_ref[h]
            new_max = jnp.maximum(old_max, jnp.max(scores, axis=0, keepdims=True))
            prob = jnp.exp(scores - new_max)
            decay = jnp.exp(old_max - new_max)
            max_ref[h] = new_max
            sum_ref[h] = sum_ref[h] * decay + jnp.sum(prob, axis=0, keepdims=True)
            prob = prob.astype(BF16)
            acc_ref[pl.ds(r0, head_dim), :] = acc_ref[pl.ds(r0, head_dim), :] * decay + (dot(vl, prob[:part], 1, 0) + dot(vr, prob[part:], 1, 0))
            return c

        return lax.fori_loop(0, heads, body, c, unroll=unroll)

    lax.fori_loop(0, half, step, 0)

    def finish(h, c):
        r0 = pl.multiple_of(h * head_dim, head_dim)
        o_ref[pl.ds(r0, head_dim), :] = (acc_ref[pl.ds(r0, head_dim), :] / sum_ref[h]).astype(BF16)
        lse_ref[h] = max_ref[h] + jnp.log(sum_ref[h])
        return c

    lax.fori_loop(0, heads, finish, 0)

    def drain(t, c):
        hop(kv_ref, me, t, to_left, from_right, left).wait_send()

        @pl.when(t < half - 1)
        def _():
            hop(kv_ref, me, t, to_right, from_left, right).wait_send()
        return c

    lax.fori_loop(0, half, drain, 0)


def attention_forward(kv_t, key_bias, qt_ext, nodes, heads, head_dim, unroll=4):
    part = kv_t.shape[1]
    rows = qt_ext.shape[1]
    half = nodes // 2
    wide = jax.ShapeDtypeStruct((nodes, LANES, part), BF16)
    sems = lambda: pltpu.SemaphoreType.DMA((half,))
    return pl.pallas_call(
        functools.partial(forward_kernel, nodes=nodes, heads=heads, head_dim=head_dim, unroll=unroll),
        in_specs=[pl.BlockSpec(memory_space=pltpu.VMEM)] * 3,
        out_specs=[pl.BlockSpec(memory_space=pltpu.VMEM)] * 4,
        out_shape=[jax.ShapeDtypeStruct((heads * head_dim, rows), BF16), jax.ShapeDtypeStruct((heads, 1, rows), F32), wide, wide],
        scratch_shapes=[
            pltpu.VMEM((nodes, 2 * head_dim, part), BF16),
            pltpu.VMEM((2 * part, LANES), BF16),
            pltpu.VMEM((heads, 1, rows), F32),
            pltpu.VMEM((heads, 1, rows), F32),
            pltpu.VMEM((heads * head_dim, rows), F32),
            sems(), sems(), sems(), sems(),
        ],
        compiler_params=pltpu.CompilerParams(vmem_limit_bytes=40 * 2**20, collective_id=3, has_side_effects=True),
        cost_estimate=pl.CostEstimate(flops=4 * heads * rows * nodes * part * head_dim, bytes_accessed=2**23, transcendentals=heads * rows * nodes * part),
        name='attention_forward',
    )(kv_t, key_bias, qt_ext)


def backward_kernel(kt_ref, vt_ref, q_ref, do_ref, qt_ref, dot_ref, dkv_ref, dq_ref, sums_r, sums_l, send_r, recv_r, send_l, recv_l, *, nodes, heads, head_dim, unroll):
    bk = kt_ref.shape[-1]
    me = lax.axis_index('nodes')
    right, left = lax.rem(me + 1, nodes), lax.rem(me + nodes - 1, nodes)
    barrier = pltpu.get_barrier_semaphore()
    for neighbour in (left, right):
        pl.semaphore_signal(barrier, inc=1, device_id={'nodes': neighbour}, device_id_type=MESH)
    pl.semaphore_wait(barrier, 2)
    dq_ref[...] = jnp.zeros_like(dq_ref)

    half = bk // 2
    rings = ((sums_r, send_r, recv_r, right, slice(0, half)), (sums_l, send_l, recv_l, left, slice(half, bk)))

    def hop(ring, t):
        sums, send_sem, recv_sem, to, cols = ring
        return pltpu.make_async_remote_copy(src_ref=sums.at[t], dst_ref=sums.at[t + 1], send_sem=send_sem.at[t], recv_sem=recv_sem.at[t + 1], device_id={'nodes': to}, device_id_type=MESH)

    def step(t, c):
        jr = lax.rem(me + 2 * nodes - 1 - t, nodes)
        jl = lax.rem(me + 1 + t, nodes)
        kt = jnp.concatenate([kt_ref[jr, :, :half], kt_ref[jl, :, half:]], axis=1)
        vt = jnp.concatenate([vt_ref[jr, :, :half], vt_ref[jl, :, half:]], axis=1)
        k_top = kt[:head_dim]

        def body(h, carry):
            dk, dv = carry
            lo = pl.multiple_of(h * LANES, LANES)
            r0 = pl.multiple_of(h * head_dim, head_dim)
            prob = jnp.exp(dot(q_ref[:, pl.ds(lo, LANES)], kt, 1, 0))
            d_prob = dot(do_ref[:, pl.ds(lo, LANES)], vt, 1, 0)
            d_scores = (prob * d_prob).astype(BF16)
            dv = dv + dot(dot_ref[pl.ds(r0, head_dim), :], prob.astype(BF16), 1, 0)
            dk = dk + dot(qt_ref[pl.ds(lo, head_dim), :], d_scores, 1, 0)
            dq_ref[pl.ds(r0, head_dim), :] += dot(k_top, d_scores, 1, 1)
            return dk, dv

        zero = jnp.zeros((head_dim, bk), F32)
        dk, dv = lax.fori_loop(0, heads, body, (zero, zero), unroll=unroll)

        @pl.when(t == 0)
        def _():
            for ring in rings:
                ring[0][t, :head_dim, :] = dk[:, ring[4]]
                ring[0][t, head_dim:, :] = dv[:, ring[4]]

        @pl.when(t > 0)
        def _():
            for ring in rings:
                hop(ring, t - 1).wait_recv()
                ring[0][t, :head_dim, :] += dk[:, ring[4]]
                ring[0][t, head_dim:, :] += dv[:, ring[4]]

        @pl.when(t < nodes - 1)
        def _():
            for ring in rings:
                hop(ring, t).start()
        return c

    lax.fori_loop(0, nodes, step, 0)

    def finish(t, c):
        for ring in rings:
            hop(ring, t).wait_send()
        return c

    lax.fori_loop(0, nodes - 1, finish, 0)
    for ring in rings:
        dkv_ref[:, ring[4]] = ring[0][nodes - 1].astype(BF16)


def attention_backward(kt_ext, vt_ext, q_ext, do_ext, qt_ext, do_t, heads, head_dim, unroll=4):
    nodes, wide, bk = kt_ext.shape
    rows = q_ext.shape[0]
    return pl.pallas_call(
        functools.partial(backward_kernel, nodes=nodes, heads=heads, head_dim=head_dim, unroll=unroll),
        in_specs=[pl.BlockSpec(memory_space=pltpu.VMEM)] * 6,
        out_specs=[pl.BlockSpec(memory_space=pltpu.VMEM)] * 2,
        out_shape=[jax.ShapeDtypeStruct((2 * head_dim, bk), BF16), jax.ShapeDtypeStruct((heads * head_dim, rows), F32)],
        scratch_shapes=[pltpu.VMEM((nodes, 2 * head_dim, bk // 2), F32)] * 2 + [pltpu.SemaphoreType.DMA((nodes,))] * 4,
        compiler_params=pltpu.CompilerParams(vmem_limit_bytes=40 * 2**20, collective_id=0, has_side_effects=True),
        cost_estimate=pl.CostEstimate(flops=10 * heads * rows * nodes * bk * head_dim, bytes_accessed=2**24, transcendentals=heads * rows * nodes * bk),
        name='attention_backward',
    )(kt_ext, vt_ext, q_ext, do_ext, qt_ext, do_t)


def reduce_kernel(x_ref, out_ref, half, parts, pair_send, pair_recv, part_send, part_recv, full_send, full_recv, back_send, back_recv, *, nodes):
    me = lax.axis_index('nodes')
    chips = nodes // 2
    core = lax.rem(me, 2)
    chip = me // 2
    partner = me + 1 - 2 * core
    rows = x_ref.shape[0]
    hr = rows // 2
    pr = hr // chips
    mine = pl.multiple_of(core * hr, hr)
    other = pl.multiple_of((1 - core) * hr, hr)

    def peer(k):
        return lax.rem(chip + k, chips)

    barrier = pltpu.get_barrier_semaphore()
    pl.semaphore_signal(barrier, inc=1, device_id={'nodes': partner}, device_id_type=MESH)
    for k in range(1, chips):
        pl.semaphore_signal(barrier, inc=1, device_id={'nodes': 2 * peer(k) + core}, device_id_type=MESH)
    pl.semaphore_wait(barrier, chips)

    swap = pltpu.make_async_remote_copy(src_ref=x_ref.at[pl.ds(other, hr)], dst_ref=half, send_sem=pair_send, recv_sem=pair_recv, device_id={'nodes': partner}, device_id_type=MESH)
    swap.start()
    swap.wait_recv()
    half[...] += x_ref[pl.ds(mine, hr)]

    def scatter(k):
        to = peer(k)
        return pltpu.make_async_remote_copy(src_ref=half.at[pl.ds(pl.multiple_of(to * pr, pr), pr)], dst_ref=parts.at[k], send_sem=part_send.at[k], recv_sem=part_recv.at[k], device_id={'nodes': 2 * to + core}, device_id_type=MESH)

    for k in range(1, chips):
        scatter(k).start()
    total = half[pl.ds(pl.multiple_of(chip * pr, pr), pr)]
    for k in range(1, chips):
        scatter(k).wait_recv()
        total = total + parts[k]
    own = pl.multiple_of(core * hr + chip * pr, pr)
    out_ref[pl.ds(own, pr)] = total

    def spread(k):
        return pltpu.make_async_remote_copy(src_ref=out_ref.at[pl.ds(own, pr)], dst_ref=out_ref.at[pl.ds(own, pr)], send_sem=full_send.at[k], recv_sem=full_recv.at[k], device_id={'nodes': 2 * peer(k) + core}, device_id_type=MESH)

    def back(k):
        at = pl.multiple_of(core * hr + lax.rem(chip + chips - k, chips) * pr, pr)
        return pltpu.make_async_remote_copy(src_ref=out_ref.at[pl.ds(at, pr)], dst_ref=out_ref.at[pl.ds(at, pr)], send_sem=back_send.at[k], recv_sem=back_recv.at[k], device_id={'nodes': partner}, device_id_type=MESH)

    for k in range(1, chips):
        spread(k).start()
    back(0).start()
    for k in range(1, chips):
        spread(k).wait_recv()
        back(k).start()
    for k in range(chips):
        back(k).wait_recv()
    swap.wait_send()
    for k in range(1, chips):
        scatter(k).wait_send()
        spread(k).wait_send()
    for k in range(chips):
        back(k).wait_send()


def reduce_all(x, nodes):
    rows, cols = x.shape
    chips = nodes // 2
    pr = rows // nodes
    sems = lambda: pltpu.SemaphoreType.DMA((chips,))
    return pl.pallas_call(
        functools.partial(reduce_kernel, nodes=nodes),
        in_specs=[pl.BlockSpec(memory_space=pltpu.VMEM)],
        out_specs=pl.BlockSpec(memory_space=pltpu.VMEM),
        out_shape=jax.ShapeDtypeStruct(x.shape, F32),
        scratch_shapes=[pltpu.VMEM((rows // 2, cols), F32), pltpu.VMEM((chips, pr, cols), F32), pltpu.SemaphoreType.DMA, pltpu.SemaphoreType.DMA, sems(), sems(), sems(), sems(), sems(), sems()],
        compiler_params=pltpu.CompilerParams(vmem_limit_bytes=16 * 2**20, collective_id=1, has_side_effects=True),
        cost_estimate=pl.CostEstimate(flops=10**10, bytes_accessed=2**23, transcendentals=0),
        name='reduce_all',
    )(x)


def one_hot(index, size):
    return (lax.broadcasted_iota(jnp.int32, (size, index.size), 0) == index[None, :]).astype(BF16)


def exchange(rows, send_ix, recv_ix, nodes):
    count, width = rows.shape
    capacity = count // nodes + count // (2 * nodes)
    picked = dot(one_hot(send_ix, nodes * capacity), rows, 1, 0).astype(BF16)
    landed = lax.all_to_all(picked.reshape(nodes, capacity, width), 'nodes', 0, 0, tiled=True)
    return dot(one_hot(recv_ix, nodes * capacity), landed.reshape(nodes * capacity, width), 0, 0).astype(BF16)


def split3(x):
    keep = lambda a: lax.reduce_precision(a, 8, 7)
    hi = keep(x)
    mid = keep(x - hi)
    return jnp.concatenate([hi, mid, keep(x - hi - mid)], axis=0).astype(BF16)


def pad_heads(w, heads, axis):
    if axis == 1:
        w3 = w.reshape(w.shape[0], heads, -1)
        return jnp.pad(w3, ((0, 0), (0, 0), (0, LANES - w3.shape[2]))).reshape(w.shape[0], heads * LANES)
    w3 = w.reshape(heads, -1, w.shape[1])
    return jnp.pad(w3, ((0, 0), (0, LANES - w3.shape[1]), (0, 0))).reshape(heads * LANES, w.shape[1])


def extra_columns(parts, heads, first):
    r = lax.broadcasted_iota(jnp.int32, (3 * heads, heads * LANES), 0)
    c = lax.broadcasted_iota(jnp.int32, (3 * heads, heads * LANES), 1)
    place = (r % heads == c // LANES) & (c % LANES == first + r // heads)
    return dot(parts, place.astype(BF16), 0, 0)


def solution(mesh):
    nodes = mesh.shape['nodes']
    row_spec = P(('graphs', 'nodes'), None)
    flat_spec = P(('graphs', 'nodes'))
    halo_spec = P(('graphs', 'nodes'), None, None)
    grad_spec = P('graphs', None)

    def device_step(x_feat, valid, halo_slot, edge_src, edge_dst, edge_mask, bal_perm, pos_enc, y_cot, w_msg, w_self, w_q, w_k, w_v, w_o, w_up, w_down):
        rows_dev, width = x_feat.shape
        head_dim = w_k.shape[1]
        heads = width // head_dim
        scale = head_dim ** -0.5
        halo_rows = halo_slot.size

        count = jnp.sum((valid > 0).astype(jnp.int32))
        info = jnp.concatenate([bal_perm, jnp.broadcast_to(count, (LANES,))])[None, None, :]
        halo_ask = jnp.pad(halo_slot.reshape(nodes, 1, -1), ((0, 0), (0, 0), (0, LANES - halo_rows // nodes)))
        live_dst = jnp.where(edge_mask.reshape(-1) > 0, edge_dst.reshape(-1), -1)
        x_bal, adjacency, bal_ix, part_ix, info_all, halo_got = entry(x_feat, info, halo_ask, edge_src.reshape(-1), live_dst, nodes)
        bal_ix, part_ix = bal_ix.reshape(-1), part_ix.reshape(-1)
        bal_all = info_all[:, 0, :rows_dev]
        owner_all = bal_all // rows_dev
        limit = jnp.sum(jnp.where(owner_all[:, :, None] == jnp.arange(nodes, dtype=jnp.int32), info_all[None, None, :, 0, rows_dev], 0), axis=2)
        key_bias = jnp.where(bal_all % rows_dev < limit, 0.0, NEG_FILL)[:, None, :]

        hidden_in = (x_bal.astype(F32) + pos_enc.astype(F32)).astype(BF16)
        w_kv = jnp.concatenate([w_k, w_v], axis=1)
        kv_t = dot(w_kv, hidden_in, 0, 1).astype(BF16)
        wq_pad = pad_heads((w_q.astype(F32) * scale).astype(BF16), heads, 1)
        row_one = (lax.broadcasted_iota(jnp.int32, (heads * LANES, 1), 0) % LANES == head_dim).astype(F32)
        qt_ext = (dot(wq_pad, hidden_in, 0, 1) + row_one).astype(BF16)

        halo_got = halo_got[:, 0, :halo_rows // nodes].reshape(-1)
        halo_pick = one_hot(halo_got, rows_dev)
        halo_send = dot(halo_pick, x_feat, 0, 0).astype(BF16)
        halo_feat = lax.all_to_all(halo_send.reshape(nodes, -1, width), 'nodes', 0, 0, tiled=True).reshape(halo_rows, width)
        adj_own, adj_halo = adjacency[:, :rows_dev], adjacency[:, rows_dev:]
        agg_msg = (dot(adj_own, x_feat, 1, 0) + dot(adj_halo, halo_feat, 1, 0)).astype(BF16)
        pre_act = dot(agg_msg, w_msg, 1, 0) + dot(x_feat, w_self, 1, 0)

        mixed_t, log_norm, kt_ext, vt_ext = attention_forward(kv_t, key_bias, qt_ext, nodes, heads, head_dim)
        u_bal = dot(mixed_t, w_o, 0, 0).astype(BF16)
        u_part = exchange(u_bal, bal_ix, part_ix, nodes)

        x_wide = x_feat.astype(F32)
        z_mid = (x_wide + jax.nn.relu(pre_act) + x_wide + u_part.astype(F32)).astype(BF16)
        h_pre = dot(z_mid, w_up, 1, 0)
        hidden = jax.nn.gelu(h_pre).astype(BF16)
        keep_row = valid[:, None] > 0
        y_out = jnp.where(keep_row, z_mid.astype(F32) + dot(hidden, w_down, 1, 0), 0.0).astype(BF16)

        g_out = jnp.where(keep_row, y_cot, jnp.zeros_like(y_cot))
        d_hidden = dot(g_out, w_down, 1, 1).astype(BF16)
        gelu_pull = jax.vjp(jax.nn.gelu, h_pre)[1]
        d_hpre = gelu_pull(d_hidden.astype(F32))[0].astype(BF16)
        d_z = (g_out.astype(F32) + dot(d_hpre, w_up, 1, 1)).astype(BF16)
        d_u = exchange(d_z, part_ix, bal_ix, nodes)

        grad_down = dot(hidden, g_out, 0, 0)
        grad_up = dot(z_mid, d_hpre, 0, 0)
        d_pre = jnp.where(pre_act > 0, d_z, jnp.zeros_like(d_z))
        grad_self = dot(x_feat, d_pre, 0, 0)
        grad_msg = dot(agg_msg, d_pre, 0, 0)
        grad_o = dot(mixed_t, d_u, 1, 0)
        grad_msg, grad_self, grad_o, grad_up, grad_down = lax.psum((grad_msg, grad_self, grad_o, grad_up, grad_down), 'nodes')

        do_t = dot(w_o, d_u, 1, 1).astype(BF16)
        delta = jnp.sum((do_t.astype(F32) * mixed_t.astype(F32)).reshape(heads, head_dim, rows_dev), axis=1)
        do_ext = (dot(d_u, pad_heads(w_o, heads, 0), 1, 1) + extra_columns(split3(-delta), heads, head_dim)).astype(BF16)
        col_one = (lax.broadcasted_iota(jnp.int32, (1, heads * LANES), 1) % LANES == head_dim).astype(F32)
        q_ext = (dot(hidden_in, wq_pad, 1, 0) + col_one + extra_columns(split3(-log_norm.reshape(heads, rows_dev)), heads, head_dim + 1)).astype(BF16)
        dkv_t, dq_t = attention_backward(kt_ext, vt_ext, q_ext, do_ext, qt_ext, do_t, heads, head_dim)
        dq_t = (dq_t * scale).astype(BF16)

        d_agg = dot(d_pre, w_msg, 1, 1).astype(BF16)
        d_halo = dot(adj_halo, d_agg, 0, 0).astype(BF16)
        halo_landed = lax.all_to_all(d_halo.reshape(nodes, -1, width), 'nodes', 0, 0, tiled=True).reshape(halo_rows, width)
        local_part = 2.0 * d_z.astype(F32) + dot(d_pre, w_self, 1, 1) + dot(adj_own, d_agg, 0, 0) + dot(halo_pick, halo_landed, 1, 0)

        grad_q = dot(hidden_in, dq_t, 0, 1)
        grad_kv = dot(hidden_in, dkv_t, 0, 1)
        dx_bal = dot(jnp.concatenate([dq_t, dkv_t], axis=0), jnp.concatenate([w_q, w_kv], axis=1), 0, 1).astype(BF16)
        attn_back = exchange(dx_bal, bal_ix, part_ix, nodes)
        dx_feat = (local_part + attn_back.astype(F32)).astype(BF16)
        late = reduce_all(jnp.concatenate([grad_q, grad_kv], axis=1), nodes)
        grad_q, grad_k, grad_v = late[:, :width], late[:, width:width + head_dim], late[:, width + head_dim:]
        return y_out, dx_feat, grad_msg, grad_self, grad_q, grad_k, grad_v, grad_o, grad_up, grad_down

    return jax.shard_map(device_step, mesh=mesh, in_specs=(row_spec, flat_spec, halo_spec, row_spec, row_spec, row_spec, flat_spec, row_spec, row_spec) + (P(),) * 8, out_specs=(row_spec, row_spec) + (grad_spec,) * 8, check_vma=False)
```

```python
import functools
import jax
import jax.numpy as jnp
from jax import lax
from jax.experimental import pallas as pl
from jax.experimental.pallas import tpu as pltpu
from jax.sharding import PartitionSpec as P

F32 = jnp.float32
BF16 = jnp.bfloat16
NEG_FILL = -1e30
LANES = 128
MESH = pl.DeviceIdType.MESH


def dot(a, b, ca, cb):
    return lax.dot_general(a, b, (((ca,), (cb,)), ((), ())), preferred_element_type=F32)


def entry_kernel(x_ref, info_ref, halo_ref, src_ref, dst_ref, x_bal_ref, adj_ref, bal_ix_ref, part_ix_ref, info_all, halo_got, acc_ref, own_ref, rank_ref, send_buf, recv_buf, info_send, info_recv, halo_send, halo_recv, row_send, row_recv, *, nodes):
    me = lax.axis_index('nodes')
    rows = x_ref.shape[0]
    cols = adj_ref.shape[1]
    steps, chunk = src_ref.shape
    capacity = send_buf.shape[1]
    peer = lambda k: lax.rem(me + k, nodes)
    barrier = pltpu.get_barrier_semaphore()

    def greet(k, c):
        pl.semaphore_signal(barrier, inc=1, device_id={'nodes': peer(k)}, device_id_type=MESH)
        return c

    lax.fori_loop(1, nodes, greet, 0)
    acc_ref[...] = jnp.zeros_like(acc_ref)
    dst_iota = lax.broadcasted_iota(jnp.int32, (rows, chunk), 0)
    src_iota = lax.broadcasted_iota(jnp.int32, (cols, chunk), 0)

    def count(i, c):
        left = jnp.where(dst_iota == dst_ref[pl.ds(i, 1), :], 1.0, 0.0).astype(BF16)
        right = jnp.where(src_iota == src_ref[pl.ds(i, 1), :], 1.0, 0.0).astype(BF16)
        acc_ref[...] += dot(left, right, 1, 1)
        return c

    first, second = steps // 10, steps // 2
    lax.fori_loop(0, first, count, 0)
    pl.semaphore_wait(barrier, nodes - 1)

    def tell(k):
        return pltpu.make_async_remote_copy(src_ref=info_ref.at[0], dst_ref=info_all.at[me], send_sem=info_send.at[k], recv_sem=info_recv.at[k], device_id={'nodes': peer(k)}, device_id_type=MESH)

    def ask(k):
        return pltpu.make_async_remote_copy(src_ref=halo_ref.at[peer(k)], dst_ref=halo_got.at[me], send_sem=halo_send.at[k], recv_sem=halo_recv.at[k], device_id={'nodes': peer(k)}, device_id_type=MESH)

    def give(k):
        return pltpu.make_async_remote_copy(src_ref=send_buf.at[k], dst_ref=recv_buf.at[me], send_sem=row_send.at[k], recv_sem=row_recv.at[k], device_id={'nodes': peer(k)}, device_id_type=MESH)

    def start_info(k, c):
        tell(k).start()
        ask(k).start()
        return c

    lax.fori_loop(1, nodes, start_info, 0)
    info_all[me] = info_ref[0]
    halo_got[me] = halo_ref[me]
    lax.fori_loop(first, second, count, 0)

    def wait_info(k, c):
        tell(k).wait_recv()
        return c

    lax.fori_loop(1, nodes, wait_info, 0)

    def mark(q, c):
        own_ref[pl.ds(q, 1), :] = jnp.where(lax.div(info_all[q][:, :rows], rows) == me, 1.0, 0.0)
        return c

    lax.fori_loop(0, nodes, mark, 0)
    before = jnp.where(lax.broadcasted_iota(jnp.int32, (rows, rows), 0) < lax.broadcasted_iota(jnp.int32, (rows, rows), 1), 1.0, 0.0).astype(BF16)
    rank_ref[...] = dot(own_ref[...].astype(BF16), before, 1, 0)
    slot_iota = lax.broadcasted_iota(jnp.int32, (rows, rows), 0)
    cap_iota = lax.broadcasted_iota(jnp.int32, (capacity, rows), 0)
    x = x_ref[...]

    def pick_rows(k, part_ix):
        q = peer(k)
        perm = info_all[q][:, :rows]
        own = lax.div(perm, rows) == me
        rank = jnp.where(own, rank_ref[pl.ds(q, 1), :].astype(jnp.int32), -1)
        ranked = jnp.where(cap_iota == rank, 1.0, 0.0).astype(BF16)
        placed = jnp.where(slot_iota == lax.rem(perm, rows), 1.0, 0.0).astype(BF16)
        pick = dot(ranked, placed, 1, 1)
        send_buf[k] = dot(pick.astype(BF16), x, 1, 0).astype(BF16)

        @pl.when(k > 0)
        def _():
            give(k).start()

        code = (cap_iota + q * capacity).astype(F32)
        return part_ix + jnp.sum(pick * code, axis=0, keepdims=True)

    part_ix = lax.fori_loop(0, nodes, pick_rows, jnp.zeros((1, rows), F32))
    part_ix_ref[...] = part_ix.astype(jnp.int32)
    recv_buf[me] = send_buf[0]
    lax.fori_loop(second, steps, count, 0)
    adj_ref[...] = acc_ref[...].astype(BF16)

    owner = lax.div(info_ref[0][:, :rows], rows)
    owners = lax.broadcasted_iota(jnp.int32, (nodes, rows), 0) == owner
    ranks = dot(jnp.where(owners, 1.0, 0.0).astype(BF16), before, 1, 0)
    bal_ix = owner * capacity + jnp.sum(jnp.where(owners, ranks, 0.0), axis=0, keepdims=True).astype(jnp.int32)
    bal_ix_ref[...] = bal_ix

    def wait_rows(k, c):
        give(k).wait_recv()
        ask(k).wait_recv()
        return c

    lax.fori_loop(1, nodes, wait_rows, 0)
    landed = jnp.where(lax.broadcasted_iota(jnp.int32, (nodes * capacity, rows), 0) == bal_ix, 1.0, 0.0).astype(BF16)
    x_bal_ref[...] = dot(landed, recv_buf[...].reshape(nodes * capacity, x.shape[1]), 0, 0).astype(BF16)

    def wait_sends(k, c):
        tell(k).wait_send()
        ask(k).wait_send()
        give(k).wait_send()
        return c

    lax.fori_loop(1, nodes, wait_sends, 0)


def entry(x, info, halo, edge_src, edge_dst, nodes, chunk=2560):
    rows, width = x.shape
    edges = edge_src.size
    if edges % chunk:
        chunk = LANES
    steps = edges // chunk
    capacity = rows // nodes + rows // (2 * nodes)
    cols = 2 * rows
    i32 = jnp.int32
    sems = lambda: pltpu.SemaphoreType.DMA((nodes,))
    return pl.pallas_call(
        functools.partial(entry_kernel, nodes=nodes),
        in_specs=[pl.BlockSpec(memory_space=pltpu.VMEM)] * 5,
        out_specs=[pl.BlockSpec(memory_space=pltpu.VMEM)] * 6,
        out_shape=[
            jax.ShapeDtypeStruct((rows, width), BF16),
            jax.ShapeDtypeStruct((rows, cols), BF16),
            jax.ShapeDtypeStruct((1, rows), i32),
            jax.ShapeDtypeStruct((1, rows), i32),
            jax.ShapeDtypeStruct((nodes,) + info.shape[1:], i32),
            jax.ShapeDtypeStruct(halo.shape, i32),
        ],
        scratch_shapes=[
            pltpu.VMEM((rows, cols), F32),
            pltpu.VMEM((nodes, rows), F32),
            pltpu.VMEM((nodes, rows), F32),
            pltpu.VMEM((nodes, capacity, width), BF16),
            pltpu.VMEM((nodes, capacity, width), BF16),
            sems(), sems(), sems(), sems(), sems(), sems(),
        ],
        compiler_params=pltpu.CompilerParams(vmem_limit_bytes=40 * 2**20, collective_id=2, has_side_effects=True),
        cost_estimate=pl.CostEstimate(flops=2 * edges * rows * cols, bytes_accessed=2**22, transcendentals=0),
        name='entry',
    )(x, info, halo, edge_src.reshape(steps, chunk), edge_dst.reshape(steps, chunk))


def forward_kernel(kv_ref, bias_ref, q_ref, o_ref, lse_ref, kt_ref, vt_ref, kv_all, k_pair, q_wide, max_ref, sum_ref, acc_ref, to_right, from_left, to_left, from_right, *, nodes, heads, head_dim, unroll):
    me = lax.axis_index('nodes')
    part = kv_ref.shape[1]
    rows = q_ref.shape[1]
    half = nodes // 2
    right, left = lax.rem(me + 1, nodes), lax.rem(me + nodes - 1, nodes)
    barrier = pltpu.get_barrier_semaphore()
    for neighbour in (left, right):
        pl.semaphore_signal(barrier, inc=1, device_id={'nodes': neighbour}, device_id_type=MESH)
    pl.semaphore_wait(barrier, 2)

    def hop(src, j, t, send, recv, to):
        return pltpu.make_async_remote_copy(src_ref=src, dst_ref=kv_all.at[j], send_sem=send.at[t], recv_sem=recv.at[t], device_id={'nodes': to}, device_id_type=MESH)

    hop(kv_ref, me, 0, to_left, from_right, left).start()
    hop(kv_ref, me, 0, to_right, from_left, right).start()
    kv_all[me] = kv_ref[...]
    max_ref[...] = jnp.full(max_ref.shape, -jnp.inf, F32)
    sum_ref[...] = jnp.zeros_like(sum_ref)
    acc_ref[...] = jnp.zeros_like(acc_ref)
    row_iota = lax.broadcasted_iota(jnp.int32, (head_dim, part), 0)
    v_extra = jnp.where(row_iota < 3, 1.0, 0.0).astype(BF16)

    q_extra = jnp.where(lax.broadcasted_iota(jnp.int32, (LANES - head_dim, rows), 0) == 0, 1.0, 0.0).astype(BF16)

    def fill(h, c):
        lo = pl.multiple_of(h * LANES, LANES)
        q_wide[pl.ds(lo, head_dim), :] = q_ref[pl.ds(pl.multiple_of(h * head_dim, head_dim), head_dim), :]
        q_wide[pl.ds(pl.multiple_of(lo + head_dim, head_dim), LANES - head_dim), :] = q_extra
        return c

    lax.fori_loop(0, heads, fill, 0)

    def widen(j, g):
        block = kv_all[j]
        k_extra = jnp.where(row_iota == 0, bias_ref[j], jnp.where(row_iota < 4, 1.0, 0.0)).astype(BF16)
        wide = jnp.concatenate([block[:head_dim], k_extra], axis=0)
        kt_ref[j] = wide
        vt_ref[j, :head_dim, :] = block[head_dim:]
        vt_ref[j, head_dim:, :] = v_extra
        k_pair[g * part:(g + 1) * part, :] = wide.T

    def step(t, c):
        jr = lax.rem(me + 1 + t, nodes)
        jl = lax.rem(me + nodes - t, nodes)
        hop(kv_all.at[jr], jr, t, to_left, from_right, left).wait_recv()

        @pl.when(t < half - 1)
        def _():
            hop(kv_all.at[jr], jr, t + 1, to_left, from_right, left).start()

        @pl.when(t > 0)
        def _():
            hop(kv_all.at[jl], jl, t - 1, to_right, from_left, right).wait_recv()

        @pl.when((t > 0) & (t < half - 1))
        def _():
            hop(kv_all.at[jl], jl, t, to_right, from_left, right).start()

        widen(jl, 0)
        widen(jr, 1)
        vl = kv_all[jl, head_dim:, :]
        vr = kv_all[jr, head_dim:, :]

        def body(h, c):
            lo = pl.multiple_of(h * LANES, LANES)
            r0 = pl.multiple_of(h * head_dim, head_dim)
            scores = dot(k_pair[...], q_wide[pl.ds(lo, LANES), :], 1, 0)
            old_max = max_ref[h]
            new_max = jnp.maximum(old_max, jnp.max(scores, axis=0, keepdims=True))
            prob = jnp.exp(scores - new_max)
            decay = jnp.exp(old_max - new_max)
            max_ref[h] = new_max
            sum_ref[h] = sum_ref[h] * decay + jnp.sum(prob, axis=0, keepdims=True)
            prob = prob.astype(BF16)
            acc_ref[pl.ds(r0, head_dim), :] = acc_ref[pl.ds(r0, head_dim), :] * decay + (dot(vl, prob[:part], 1, 0) + dot(vr, prob[part:], 1, 0))
            return c

        return lax.fori_loop(0, heads, body, c, unroll=unroll)

    lax.fori_loop(0, half, step, 0)

    def finish(h, c):
        r0 = pl.multiple_of(h * head_dim, head_dim)
        o_ref[pl.ds(r0, head_dim), :] = (acc_ref[pl.ds(r0, head_dim), :] / sum_ref[h]).astype(BF16)
        lse_ref[h] = max_ref[h] + jnp.log(sum_ref[h])
        return c

    lax.fori_loop(0, heads, finish, 0)

    def drain(t, c):
        hop(kv_ref, me, t, to_left, from_right, left).wait_send()

        @pl.when(t < half - 1)
        def _():
            hop(kv_ref, me, t, to_right, from_left, right).wait_send()
        return c

    lax.fori_loop(0, half, drain, 0)


def attention_forward(kv_t, key_bias, q_t, nodes, heads, head_dim, unroll=4):
    part = kv_t.shape[1]
    rows = q_t.shape[1]
    half = nodes // 2
    wide = jax.ShapeDtypeStruct((nodes, LANES, part), BF16)
    sems = lambda: pltpu.SemaphoreType.DMA((half,))
    return pl.pallas_call(
        functools.partial(forward_kernel, nodes=nodes, heads=heads, head_dim=head_dim, unroll=unroll),
        in_specs=[pl.BlockSpec(memory_space=pltpu.VMEM)] * 3,
        out_specs=[pl.BlockSpec(memory_space=pltpu.VMEM)] * 4,
        out_shape=[jax.ShapeDtypeStruct((heads * head_dim, rows), BF16), jax.ShapeDtypeStruct((heads, 1, rows), F32), wide, wide],
        scratch_shapes=[
            pltpu.VMEM((nodes, 2 * head_dim, part), BF16),
            pltpu.VMEM((2 * part, LANES), BF16),
            pltpu.VMEM((heads * LANES, rows), BF16),
            pltpu.VMEM((heads, 1, rows), F32),
            pltpu.VMEM((heads, 1, rows), F32),
            pltpu.VMEM((heads * head_dim, rows), F32),
            sems(), sems(), sems(), sems(),
        ],
        compiler_params=pltpu.CompilerParams(vmem_limit_bytes=40 * 2**20, collective_id=3, has_side_effects=True),
        cost_estimate=pl.CostEstimate(flops=4 * heads * rows * nodes * part * head_dim, bytes_accessed=2**23, transcendentals=heads * rows * nodes * part),
        name='attention_forward',
    )(kv_t, key_bias, q_t)


def backward_kernel(kt_ref, vt_ref, qt_ref, dot_ref, o_ref, lse_ref, dkv_ref, dq_ref, q_wide, do_wide, sums_r, sums_l, send_r, recv_r, send_l, recv_l, *, nodes, heads, head_dim, unroll):
    bk = kt_ref.shape[-1]
    me = lax.axis_index('nodes')
    right, left = lax.rem(me + 1, nodes), lax.rem(me + nodes - 1, nodes)
    barrier = pltpu.get_barrier_semaphore()
    for neighbour in (left, right):
        pl.semaphore_signal(barrier, inc=1, device_id={'nodes': neighbour}, device_id_type=MESH)
    dq_ref[...] = jnp.zeros_like(dq_ref)
    rows = qt_ref.shape[1]
    extra_iota = lax.broadcasted_iota(jnp.int32, (LANES - head_dim, rows), 0)

    def stack(parts):
        block = jnp.zeros((LANES - head_dim, rows), F32)
        for r, part in enumerate(parts):
            block = jnp.where(extra_iota == r, part, block)
        return block.astype(BF16)

    def split(x):
        hi = x.astype(BF16).astype(F32)
        mid = (x - hi).astype(BF16).astype(F32)
        return hi, mid, x - hi - mid

    def widen(h, c):
        r0 = pl.multiple_of(h * head_dim, head_dim)
        lo = pl.multiple_of(h * LANES, LANES)
        d_o = dot_ref[pl.ds(r0, head_dim), :]
        delta = jnp.sum(d_o.astype(F32) * o_ref[pl.ds(r0, head_dim), :].astype(F32), axis=0, keepdims=True)
        q_wide[:, pl.ds(lo, LANES)] = jnp.concatenate([qt_ref[pl.ds(r0, head_dim), :], stack((1.0,) + split(-lse_ref[h]))], axis=0).T
        do_wide[:, pl.ds(lo, LANES)] = jnp.concatenate([d_o, stack(split(-delta))], axis=0).T
        return c

    lax.fori_loop(0, heads, widen, 0)
    pl.semaphore_wait(barrier, 2)

    half = bk // 2
    rings = ((sums_r, send_r, recv_r, right, slice(0, half)), (sums_l, send_l, recv_l, left, slice(half, bk)))

    def hop(ring, t):
        sums, send_sem, recv_sem, to, cols = ring
        return pltpu.make_async_remote_copy(src_ref=sums.at[t], dst_ref=sums.at[t + 1], send_sem=send_sem.at[t], recv_sem=recv_sem.at[t + 1], device_id={'nodes': to}, device_id_type=MESH)

    def step(t, c):
        jr = lax.rem(me + 2 * nodes - 1 - t, nodes)
        jl = lax.rem(me + 1 + t, nodes)
        kt = jnp.concatenate([kt_ref[jr, :, :half], kt_ref[jl, :, half:]], axis=1)
        vt = jnp.concatenate([vt_ref[jr, :, :half], vt_ref[jl, :, half:]], axis=1)
        k_top = kt[:head_dim]

        def body(h, carry):
            dk, dv = carry
            lo = pl.multiple_of(h * LANES, LANES)
            r0 = pl.multiple_of(h * head_dim, head_dim)
            prob = jnp.exp(dot(q_wide[:, pl.ds(lo, LANES)], kt, 1, 0))
            d_prob = dot(do_wide[:, pl.ds(lo, LANES)], vt, 1, 0)
            d_scores = (prob * d_prob).astype(BF16)
            dv = dv + dot(dot_ref[pl.ds(r0, head_dim), :], prob.astype(BF16), 1, 0)
            dk = dk + dot(qt_ref[pl.ds(r0, head_dim), :], d_scores, 1, 0)
            dq_ref[pl.ds(r0, head_dim), :] += dot(k_top, d_scores, 1, 1)
            return dk, dv

        zero = jnp.zeros((head_dim, bk), F32)
        dk, dv = lax.fori_loop(0, heads, body, (zero, zero), unroll=unroll)

        @pl.when(t == 0)
        def _():
            for ring in rings:
                ring[0][t, :head_dim, :] = dk[:, ring[4]]
                ring[0][t, head_dim:, :] = dv[:, ring[4]]

        @pl.when(t > 0)
        def _():
            for ring in rings:
                hop(ring, t - 1).wait_recv()
                ring[0][t, :head_dim, :] += dk[:, ring[4]]
                ring[0][t, head_dim:, :] += dv[:, ring[4]]

        @pl.when(t < nodes - 1)
        def _():
            for ring in rings:
                hop(ring, t).start()
        return c

    lax.fori_loop(0, nodes, step, 0)

    def finish(t, c):
        for ring in rings:
            hop(ring, t).wait_send()
        return c

    lax.fori_loop(0, nodes - 1, finish, 0)
    for ring in rings:
        dkv_ref[:, ring[4]] = ring[0][nodes - 1].astype(BF16)


def attention_backward(kt_ext, vt_ext, q_t, do_t, mixed_t, log_norm, heads, head_dim, unroll=4):
    nodes, wide, bk = kt_ext.shape
    rows = q_t.shape[1]
    return pl.pallas_call(
        functools.partial(backward_kernel, nodes=nodes, heads=heads, head_dim=head_dim, unroll=unroll),
        in_specs=[pl.BlockSpec(memory_space=pltpu.VMEM)] * 6,
        out_specs=[pl.BlockSpec(memory_space=pltpu.VMEM)] * 2,
        out_shape=[jax.ShapeDtypeStruct((2 * head_dim, bk), BF16), jax.ShapeDtypeStruct((heads * head_dim, rows), F32)],
        scratch_shapes=[pltpu.VMEM((rows, heads * LANES), BF16)] * 2 + [pltpu.VMEM((nodes, 2 * head_dim, bk // 2), F32)] * 2 + [pltpu.SemaphoreType.DMA((nodes,))] * 4,
        compiler_params=pltpu.CompilerParams(vmem_limit_bytes=40 * 2**20, collective_id=0, has_side_effects=True),
        cost_estimate=pl.CostEstimate(flops=10 * heads * rows * nodes * bk * head_dim, bytes_accessed=2**24, transcendentals=heads * rows * nodes * bk),
        name='attention_backward',
    )(kt_ext, vt_ext, q_t, do_t, mixed_t, log_norm)


def exit_kernel(rows_ref, send_ix_ref, recv_ix_ref, x_ref, moved_ref, out_ref, send_buf, recv_buf, half, sums_r, sums_l, row_send, row_recv, pair_send, pair_recv, add_send_r, add_recv_r, add_send_l, add_recv_l, fill_send_r, fill_recv_r, fill_send_l, fill_recv_l, back_send_r, back_recv_r, back_send_l, back_recv_l, *, nodes):
    me = lax.axis_index('nodes')
    chips = nodes // 2
    core = lax.rem(me, 2)
    chip = me // 2
    partner = me + 1 - 2 * core
    hr = x_ref.shape[0] // 2
    pr = hr // chips
    mine = pl.multiple_of(core * hr, hr)
    other = pl.multiple_of((1 - core) * hr, hr)
    count, width = rows_ref.shape
    capacity = send_buf.shape[1]
    peer = lambda k: lax.rem(me + k, nodes)
    right = 2 * lax.rem(chip + 1, chips) + core
    left = 2 * lax.rem(chip + chips - 1, chips) + core
    barrier = pltpu.get_barrier_semaphore()

    def greet(k, c):
        pl.semaphore_signal(barrier, inc=1, device_id={'nodes': peer(k)}, device_id_type=MESH)
        return c

    lax.fori_loop(1, nodes, greet, 0)
    pl.semaphore_wait(barrier, nodes - 1)
    swap = pltpu.make_async_remote_copy(src_ref=x_ref.at[pl.ds(other, hr)], dst_ref=half, send_sem=pair_send, recv_sem=pair_recv, device_id={'nodes': partner}, device_id_type=MESH)
    swap.start()

    def give(k):
        return pltpu.make_async_remote_copy(src_ref=send_buf.at[k], dst_ref=recv_buf.at[me], send_sem=row_send.at[k], recv_sem=row_recv.at[k], device_id={'nodes': peer(k)}, device_id_type=MESH)

    cap_iota = lax.broadcasted_iota(jnp.int32, (capacity, count), 0)

    def pick_rows(k, c):
        pick = jnp.where(cap_iota + peer(k) * capacity == send_ix_ref[...], 1.0, 0.0).astype(BF16)
        send_buf[k] = dot(pick, rows_ref[...], 1, 0).astype(BF16)

        @pl.when(k > 0)
        def _():
            give(k).start()
        return c

    lax.fori_loop(0, nodes, pick_rows, 0)
    recv_buf[me] = send_buf[0]

    swap.wait_recv()
    half[...] += x_ref[pl.ds(mine, hr)]
    cut = sums_r.shape[2]
    rings = ((sums_r, 1, slice(0, cut), right, add_send_r, add_recv_r, fill_send_r, fill_recv_r, back_send_r, back_recv_r), (sums_l, chips - 1, slice(cut, x_ref.shape[1]), left, add_send_l, add_recv_l, fill_send_l, fill_recv_l, back_send_l, back_recv_l))

    def add_hop(ring, t):
        return pltpu.make_async_remote_copy(src_ref=ring[0].at[t], dst_ref=ring[0].at[t + 1], send_sem=ring[4].at[t], recv_sem=ring[5].at[t + 1], device_id={'nodes': ring[3]}, device_id_type=MESH)

    def add_step(t, c):
        for ring in rings:
            at = lax.rem(chip + (chips - ring[1]) * (t + 1), chips)
            term = half[pl.ds(pl.multiple_of(at * pr, pr), pr), ring[2]]

            @pl.when(t == 0)
            def _():
                ring[0][t] = term

            @pl.when(t > 0)
            def _():
                add_hop(ring, t - 1).wait_recv()
                ring[0][t] += term

            @pl.when(t < chips - 1)
            def _():
                add_hop(ring, t).start()
        return c

    lax.fori_loop(0, chips, add_step, 0)

    def place(t, ring):
        at = lax.rem(chip + (chips - ring[1]) * t, chips)
        return out_ref.at[pl.ds(pl.multiple_of(core * hr + at * pr, pr), pr), ring[2]]

    def fill_hop(ring, t):
        return pltpu.make_async_remote_copy(src_ref=place(t, ring), dst_ref=place(t, ring), send_sem=ring[6].at[t], recv_sem=ring[7].at[t + 1], device_id={'nodes': ring[3]}, device_id_type=MESH)

    def back_hop(ring, t):
        return pltpu.make_async_remote_copy(src_ref=place(t, ring), dst_ref=place(t, ring), send_sem=ring[8].at[t], recv_sem=ring[9].at[t], device_id={'nodes': partner}, device_id_type=MESH)

    for ring in rings:
        out_ref[pl.ds(pl.multiple_of(core * hr + chip * pr, pr), pr), ring[2]] = ring[0][chips - 1]

    def fill_step(t, c):
        for ring in rings:
            @pl.when(t > 0)
            def _():
                fill_hop(ring, t - 1).wait_recv()

            @pl.when(t < chips - 1)
            def _():
                fill_hop(ring, t).start()

            back_hop(ring, t).start()
        return c

    lax.fori_loop(0, chips, fill_step, 0)

    def wait_rows(k, c):
        give(k).wait_recv()
        return c

    lax.fori_loop(1, nodes, wait_rows, 0)
    landed = jnp.where(lax.broadcasted_iota(jnp.int32, (nodes * capacity, count), 0) == recv_ix_ref[...], 1.0, 0.0).astype(BF16)
    moved_ref[...] = dot(landed, recv_buf[...].reshape(nodes * capacity, width), 0, 0).astype(BF16)

    def wait_sends(k, c):
        give(k).wait_send()
        return c

    lax.fori_loop(1, nodes, wait_sends, 0)
    swap.wait_send()

    def drain(t, c):
        for ring in rings:
            back_hop(ring, t).wait()

            @pl.when(t < chips - 1)
            def _():
                add_hop(ring, t).wait_send()
                fill_hop(ring, t).wait_send()
        return c

    lax.fori_loop(0, chips, drain, 0)


def exit_moves(rows, send_ix, recv_ix, x, nodes):
    count, width = rows.shape
    total, cols = x.shape
    chips = nodes // 2
    pr = total // nodes
    cut = (cols // LANES + 1) // 2 * LANES
    capacity = count // nodes + count // (2 * nodes)
    row_sems = [pltpu.SemaphoreType.DMA((nodes,))] * 2
    return pl.pallas_call(
        functools.partial(exit_kernel, nodes=nodes),
        in_specs=[pl.BlockSpec(memory_space=pltpu.VMEM)] * 4,
        out_specs=[pl.BlockSpec(memory_space=pltpu.VMEM)] * 2,
        out_shape=[jax.ShapeDtypeStruct(rows.shape, BF16), jax.ShapeDtypeStruct(x.shape, F32)],
        scratch_shapes=[pltpu.VMEM((nodes, capacity, width), BF16)] * 2
        + [pltpu.VMEM((total // 2, cols), F32), pltpu.VMEM((chips, pr, cut), F32), pltpu.VMEM((chips, pr, cols - cut), F32)]
        + row_sems + [pltpu.SemaphoreType.DMA] * 2 + [pltpu.SemaphoreType.DMA((chips,))] * 12,
        compiler_params=pltpu.CompilerParams(vmem_limit_bytes=24 * 2**20, collective_id=1, has_side_effects=True),
        cost_estimate=pl.CostEstimate(flops=10**10, bytes_accessed=2**23, transcendentals=0),
        name='exit_moves',
    )(rows, send_ix.reshape(1, -1), recv_ix.reshape(1, -1), x)


def one_hot(index, size):
    return (lax.broadcasted_iota(jnp.int32, (size, index.size), 0) == index[None, :]).astype(BF16)


def exchange(rows, send_ix, recv_ix, nodes):
    count, width = rows.shape
    capacity = count // nodes + count // (2 * nodes)
    picked = dot(one_hot(send_ix, nodes * capacity), rows, 1, 0).astype(BF16)
    landed = lax.all_to_all(picked.reshape(nodes, capacity, width), 'nodes', 0, 0, tiled=True)
    return dot(one_hot(recv_ix, nodes * capacity), landed.reshape(nodes * capacity, width), 0, 0).astype(BF16)


def solution(mesh):
    nodes = mesh.shape['nodes']
    row_spec = P(('graphs', 'nodes'), None)
    flat_spec = P(('graphs', 'nodes'))
    halo_spec = P(('graphs', 'nodes'), None, None)
    grad_spec = P('graphs', None)

    def device_step(x_feat, valid, halo_slot, edge_src, edge_dst, edge_mask, bal_perm, pos_enc, y_cot, w_msg, w_self, w_q, w_k, w_v, w_o, w_up, w_down):
        rows_dev, width = x_feat.shape
        head_dim = w_k.shape[1]
        heads = width // head_dim
        scale = head_dim ** -0.5
        halo_rows = halo_slot.size

        count = jnp.sum((valid > 0).astype(jnp.int32))
        info = jnp.concatenate([bal_perm, jnp.broadcast_to(count, (LANES,))])[None, None, :]
        halo_ask = jnp.pad(halo_slot.reshape(nodes, 1, -1), ((0, 0), (0, 0), (0, LANES - halo_rows // nodes)))
        live_dst = jnp.where(edge_mask.reshape(-1) > 0, edge_dst.reshape(-1), -1)
        x_bal, adjacency, bal_ix, part_ix, info_all, halo_got = entry(x_feat, info, halo_ask, edge_src.reshape(-1), live_dst, nodes)
        bal_ix, part_ix = bal_ix.reshape(-1), part_ix.reshape(-1)
        bal_all = info_all[:, 0, :rows_dev]
        owner_all = bal_all // rows_dev
        limit = jnp.sum(jnp.where(owner_all[:, :, None] == jnp.arange(nodes, dtype=jnp.int32), info_all[None, None, :, 0, rows_dev], 0), axis=2)
        key_bias = jnp.where(bal_all % rows_dev < limit, 0.0, NEG_FILL)[:, None, :]

        hidden_in = (x_bal.astype(F32) + pos_enc.astype(F32)).astype(BF16)
        w_kv = jnp.concatenate([w_k, w_v], axis=1)
        kv_t = dot(w_kv, hidden_in, 0, 1).astype(BF16)
        q_t = dot((w_q.astype(F32) * scale).astype(BF16), hidden_in, 0, 1).astype(BF16)

        halo_got = halo_got[:, 0, :halo_rows // nodes].reshape(-1)
        halo_pick = one_hot(halo_got, rows_dev)
        halo_send = dot(halo_pick, x_feat, 0, 0).astype(BF16)
        halo_feat = lax.all_to_all(halo_send.reshape(nodes, -1, width), 'nodes', 0, 0, tiled=True).reshape(halo_rows, width)
        adj_own, adj_halo = adjacency[:, :rows_dev], adjacency[:, rows_dev:]
        agg_msg = (dot(adj_own, x_feat, 1, 0) + dot(adj_halo, halo_feat, 1, 0)).astype(BF16)
        pre_act = dot(agg_msg, w_msg, 1, 0) + dot(x_feat, w_self, 1, 0)

        mixed_t, log_norm, kt_ext, vt_ext = attention_forward(kv_t, key_bias, q_t, nodes, heads, head_dim)
        u_bal = dot(mixed_t, w_o, 0, 0).astype(BF16)
        u_part = exchange(u_bal, bal_ix, part_ix, nodes)

        x_wide = x_feat.astype(F32)
        z_mid = (x_wide + jax.nn.relu(pre_act) + x_wide + u_part.astype(F32)).astype(BF16)
        h_pre = dot(z_mid, w_up, 1, 0)
        hidden = jax.nn.gelu(h_pre).astype(BF16)
        keep_row = valid[:, None] > 0
        y_out = jnp.where(keep_row, z_mid.astype(F32) + dot(hidden, w_down, 1, 0), 0.0).astype(BF16)

        g_out = jnp.where(keep_row, y_cot, jnp.zeros_like(y_cot))
        d_hidden = dot(g_out, w_down, 1, 1).astype(BF16)
        gelu_pull = jax.vjp(jax.nn.gelu, h_pre)[1]
        d_hpre = gelu_pull(d_hidden.astype(F32))[0].astype(BF16)
        d_z = (g_out.astype(F32) + dot(d_hpre, w_up, 1, 1)).astype(BF16)
        d_u = exchange(d_z, part_ix, bal_ix, nodes)

        grad_down = dot(hidden, g_out, 0, 0)
        grad_up = dot(z_mid, d_hpre, 0, 0)
        d_pre = jnp.where(pre_act > 0, d_z, jnp.zeros_like(d_z))
        grad_self = dot(x_feat, d_pre, 0, 0)
        grad_msg = dot(agg_msg, d_pre, 0, 0)
        grad_msg, grad_self, grad_up, grad_down = lax.psum((grad_msg, grad_self, grad_up, grad_down), 'nodes')

        do_t = dot(w_o, d_u, 1, 1).astype(BF16)
        grad_o = dot(mixed_t, d_u, 1, 0)
        dkv_t, dq_t = attention_backward(kt_ext, vt_ext, q_t, do_t, mixed_t, log_norm, heads, head_dim)
        dq_t = (dq_t * scale).astype(BF16)

        d_agg = dot(d_pre, w_msg, 1, 1).astype(BF16)
        d_halo = dot(adj_halo, d_agg, 0, 0).astype(BF16)
        halo_landed = lax.all_to_all(d_halo.reshape(nodes, -1, width), 'nodes', 0, 0, tiled=True).reshape(halo_rows, width)
        local_part = 2.0 * d_z.astype(F32) + dot(d_pre, w_self, 1, 1) + dot(adj_own, d_agg, 0, 0) + dot(halo_pick, halo_landed, 1, 0)

        grad_q = dot(hidden_in, dq_t, 0, 1)
        grad_kv = dot(hidden_in, dkv_t, 0, 1)
        dx_bal = dot(jnp.concatenate([dq_t, dkv_t], axis=0), jnp.concatenate([w_q, w_kv], axis=1), 0, 1).astype(BF16)
        attn_back, late = exit_moves(dx_bal, bal_ix, part_ix, jnp.concatenate([grad_q, grad_o, grad_kv], axis=1), nodes)
        dx_feat = (local_part + attn_back.astype(F32)).astype(BF16)
        grad_q, grad_o, grad_k, grad_v = late[:, :width], late[:, width:2 * width], late[:, 2 * width:2 * width + head_dim], late[:, 2 * width + head_dim:]
        return y_out, dx_feat, grad_msg, grad_self, grad_q, grad_k, grad_v, grad_o, grad_up, grad_down

    return jax.shard_map(device_step, mesh=mesh, in_specs=(row_spec, flat_spec, halo_spec, row_spec, row_spec, row_spec, flat_spec, row_spec, row_spec) + (P(),) * 8, out_specs=(row_spec, row_spec) + (grad_spec,) * 8, check_vma=False)
```

```python
import functools
import jax
import jax.numpy as jnp
from jax import lax
from jax.experimental import pallas as pl
from jax.experimental.pallas import tpu as pltpu
from jax.sharding import PartitionSpec as P

F32 = jnp.float32
BF16 = jnp.bfloat16
NEG_FILL = -1e30
LANES = 128
MESH = pl.DeviceIdType.MESH


def dot(a, b, ca, cb):
    return lax.dot_general(a, b, (((ca,), (cb,)), ((), ())), preferred_element_type=F32)


def entry_kernel(x_ref, info_ref, halo_ref, src_ref, dst_ref, x_bal_ref, adj_ref, bal_ix_ref, part_ix_ref, info_all, halo_got, halo_rows, acc_ref, own_ref, rank_ref, send_buf, recv_buf, halo_buf, feat_send, feat_recv, info_send, info_recv, halo_send, halo_recv, row_send, row_recv, *, nodes):
    me = lax.axis_index('nodes')
    rows = x_ref.shape[0]
    cols = adj_ref.shape[1]
    steps, chunk = src_ref.shape
    capacity = send_buf.shape[1]
    peer = lambda k: lax.rem(me + k, nodes)
    barrier = pltpu.get_barrier_semaphore()

    def greet(k, c):
        pl.semaphore_signal(barrier, inc=1, device_id={'nodes': peer(k)}, device_id_type=MESH)
        return c

    lax.fori_loop(1, nodes, greet, 0)
    acc_ref[...] = jnp.zeros_like(acc_ref)
    dst_iota = lax.broadcasted_iota(jnp.int32, (rows, chunk), 0)
    src_iota = lax.broadcasted_iota(jnp.int32, (cols, chunk), 0)

    def count(i, c):
        left = jnp.where(dst_iota == dst_ref[pl.ds(i, 1), :], 1.0, 0.0).astype(BF16)
        right = jnp.where(src_iota == src_ref[pl.ds(i, 1), :], 1.0, 0.0).astype(BF16)
        acc_ref[...] += dot(left, right, 1, 1)
        return c

    first, second = steps // 10, 3 * steps // 10
    lax.fori_loop(0, first, count, 0)
    pl.semaphore_wait(barrier, nodes - 1)

    def tell(k):
        return pltpu.make_async_remote_copy(src_ref=info_ref.at[0], dst_ref=info_all.at[me], send_sem=info_send.at[k], recv_sem=info_recv.at[k], device_id={'nodes': peer(k)}, device_id_type=MESH)

    def ask(k):
        return pltpu.make_async_remote_copy(src_ref=halo_ref.at[peer(k)], dst_ref=halo_got.at[me], send_sem=halo_send.at[k], recv_sem=halo_recv.at[k], device_id={'nodes': peer(k)}, device_id_type=MESH)

    def give(k):
        return pltpu.make_async_remote_copy(src_ref=send_buf.at[k], dst_ref=recv_buf.at[me], send_sem=row_send.at[k], recv_sem=row_recv.at[k], device_id={'nodes': peer(k)}, device_id_type=MESH)

    def lend(k):
        return pltpu.make_async_remote_copy(src_ref=halo_buf.at[k], dst_ref=halo_rows.at[me], send_sem=feat_send.at[k], recv_sem=feat_recv.at[k], device_id={'nodes': peer(k)}, device_id_type=MESH)

    def start_info(k, c):
        tell(k).start()
        ask(k).start()
        return c

    lax.fori_loop(1, nodes, start_info, 0)
    info_all[me] = info_ref[0]
    halo_got[me] = halo_ref[me]
    lax.fori_loop(first, second, count, 0)

    def wait_info(k, c):
        tell(k).wait_recv()
        return c

    lax.fori_loop(1, nodes, wait_info, 0)

    def mark(q, c):
        own_ref[pl.ds(q, 1), :] = jnp.where(lax.div(info_all[q][:, :rows], rows) == me, 1.0, 0.0)
        return c

    lax.fori_loop(0, nodes, mark, 0)
    before = jnp.where(lax.broadcasted_iota(jnp.int32, (rows, rows), 0) < lax.broadcasted_iota(jnp.int32, (rows, rows), 1), 1.0, 0.0).astype(BF16)
    rank_ref[...] = dot(own_ref[...].astype(BF16), before, 1, 0)
    slot_iota = lax.broadcasted_iota(jnp.int32, (rows, rows), 0)
    cap_iota = lax.broadcasted_iota(jnp.int32, (capacity, rows), 0)
    x = x_ref[...]

    def pick_rows(k, part_ix):
        q = peer(k)
        perm = info_all[q][:, :rows]
        own = lax.div(perm, rows) == me
        rank = jnp.where(own, rank_ref[pl.ds(q, 1), :].astype(jnp.int32), -1)
        ranked = jnp.where(cap_iota == rank, 1.0, 0.0).astype(BF16)
        placed = jnp.where(slot_iota == lax.rem(perm, rows), 1.0, 0.0).astype(BF16)
        pick = dot(ranked, placed, 1, 1)
        send_buf[k] = dot(pick.astype(BF16), x, 1, 0).astype(BF16)

        @pl.when(k > 0)
        def _():
            give(k).start()

        code = (cap_iota + q * capacity).astype(F32)
        return part_ix + jnp.sum(pick * code, axis=0, keepdims=True)

    part_ix = lax.fori_loop(0, nodes, pick_rows, jnp.zeros((1, rows), F32))
    want_iota = lax.broadcasted_iota(jnp.int32, (rows, LANES), 0)

    def pick_halo(k, c):
        @pl.when(k > 0)
        def _():
            pltpu.make_async_remote_copy(src_ref=halo_ref.at[me], dst_ref=halo_got.at[me], send_sem=halo_send.at[k], recv_sem=halo_recv.at[lax.rem(nodes - k, nodes)], device_id={'nodes': peer(k)}, device_id_type=MESH).wait_recv()

        placed = jnp.where(want_iota == halo_got[peer(k)], 1.0, 0.0).astype(BF16)
        halo_buf[k] = dot(placed, x, 0, 0)[:halo_buf.shape[1]].astype(BF16)

        @pl.when(k > 0)
        def _():
            lend(k).start()
        return c

    lax.fori_loop(0, nodes, pick_halo, 0)
    halo_rows[me] = halo_buf[0]
    part_ix_ref[...] = part_ix.astype(jnp.int32)
    recv_buf[me] = send_buf[0]
    lax.fori_loop(second, steps, count, 0)
    adj_ref[...] = acc_ref[...].astype(BF16)

    owner = lax.div(info_ref[0][:, :rows], rows)
    owners = lax.broadcasted_iota(jnp.int32, (nodes, rows), 0) == owner
    ranks = dot(jnp.where(owners, 1.0, 0.0).astype(BF16), before, 1, 0)
    bal_ix = owner * capacity + jnp.sum(jnp.where(owners, ranks, 0.0), axis=0, keepdims=True).astype(jnp.int32)
    bal_ix_ref[...] = bal_ix

    def wait_rows(k, c):
        give(k).wait_recv()
        return c

    lax.fori_loop(1, nodes, wait_rows, 0)
    landed = jnp.where(lax.broadcasted_iota(jnp.int32, (nodes * capacity, rows), 0) == bal_ix, 1.0, 0.0).astype(BF16)
    x_bal_ref[...] = dot(landed, recv_buf[...].reshape(nodes * capacity, x.shape[1]), 0, 0).astype(BF16)

    def wait_sends(k, c):
        lend(k).wait_recv()
        tell(k).wait_send()
        ask(k).wait_send()
        give(k).wait_send()
        lend(k).wait_send()
        return c

    lax.fori_loop(1, nodes, wait_sends, 0)


def entry(x, info, halo, per_pair, edge_src, edge_dst, nodes, chunk=2560):
    rows, width = x.shape
    edges = edge_src.size
    if edges % chunk:
        chunk = LANES
    steps = edges // chunk
    capacity = rows // nodes + rows // (2 * nodes)
    cols = 2 * rows
    i32 = jnp.int32
    sems = lambda: pltpu.SemaphoreType.DMA((nodes,))
    return pl.pallas_call(
        functools.partial(entry_kernel, nodes=nodes),
        in_specs=[pl.BlockSpec(memory_space=pltpu.VMEM)] * 5,
        out_specs=[pl.BlockSpec(memory_space=pltpu.VMEM)] * 7,
        out_shape=[
            jax.ShapeDtypeStruct((rows, width), BF16),
            jax.ShapeDtypeStruct((rows, cols), BF16),
            jax.ShapeDtypeStruct((1, rows), i32),
            jax.ShapeDtypeStruct((1, rows), i32),
            jax.ShapeDtypeStruct((nodes,) + info.shape[1:], i32),
            jax.ShapeDtypeStruct(halo.shape, i32),
            jax.ShapeDtypeStruct((nodes, per_pair, width), BF16),
        ],
        scratch_shapes=[
            pltpu.VMEM((rows, cols), F32),
            pltpu.VMEM((nodes, rows), F32),
            pltpu.VMEM((nodes, rows), F32),
            pltpu.VMEM((nodes, capacity, width), BF16),
            pltpu.VMEM((nodes, capacity, width), BF16),
            pltpu.VMEM((nodes, per_pair, width), BF16),
            sems(), sems(), sems(), sems(), sems(), sems(), sems(), sems(),
        ],
        compiler_params=pltpu.CompilerParams(vmem_limit_bytes=40 * 2**20, collective_id=2, has_side_effects=True),
        cost_estimate=pl.CostEstimate(flops=2 * edges * rows * cols, bytes_accessed=2**22, transcendentals=0),
        name='entry',
    )(x, info, halo, edge_src.reshape(steps, chunk), edge_dst.reshape(steps, chunk))


def forward_kernel(kv_ref, bias_ref, q_ref, o_ref, lse_ref, kt_ref, vt_ref, kv_all, k_pair, q_wide, max_ref, sum_ref, acc_ref, to_right, from_left, to_left, from_right, *, nodes, heads, head_dim, unroll):
    me = lax.axis_index('nodes')
    part = kv_ref.shape[1]
    rows = q_ref.shape[1]
    half = nodes // 2
    right, left = lax.rem(me + 1, nodes), lax.rem(me + nodes - 1, nodes)
    barrier = pltpu.get_barrier_semaphore()
    for neighbour in (left, right):
        pl.semaphore_signal(barrier, inc=1, device_id={'nodes': neighbour}, device_id_type=MESH)
    pl.semaphore_wait(barrier, 2)

    def hop(src, j, t, send, recv, to):
        return pltpu.make_async_remote_copy(src_ref=src, dst_ref=kv_all.at[j], send_sem=send.at[t], recv_sem=recv.at[t], device_id={'nodes': to}, device_id_type=MESH)

    hop(kv_ref, me, 0, to_left, from_right, left).start()
    hop(kv_ref, me, 0, to_right, from_left, right).start()
    kv_all[me] = kv_ref[...]
    max_ref[...] = jnp.full(max_ref.shape, -jnp.inf, F32)
    sum_ref[...] = jnp.zeros_like(sum_ref)
    acc_ref[...] = jnp.zeros_like(acc_ref)
    row_iota = lax.broadcasted_iota(jnp.int32, (head_dim, part), 0)
    v_extra = jnp.where(row_iota < 3, 1.0, 0.0).astype(BF16)

    q_extra = jnp.where(lax.broadcasted_iota(jnp.int32, (LANES - head_dim, rows), 0) == 0, 1.0, 0.0).astype(BF16)

    def fill(h, c):
        lo = pl.multiple_of(h * LANES, LANES)
        q_wide[pl.ds(lo, head_dim), :] = q_ref[pl.ds(pl.multiple_of(h * head_dim, head_dim), head_dim), :]
        q_wide[pl.ds(pl.multiple_of(lo + head_dim, head_dim), LANES - head_dim), :] = q_extra
        return c

    lax.fori_loop(0, heads, fill, 0)

    def widen(j, g):
        block = kv_all[j]
        k_extra = jnp.where(row_iota == 0, bias_ref[j], jnp.where(row_iota < 4, 1.0, 0.0)).astype(BF16)
        wide = jnp.concatenate([block[:head_dim], k_extra], axis=0)
        kt_ref[j] = wide
        vt_ref[j, :head_dim, :] = block[head_dim:]
        vt_ref[j, head_dim:, :] = v_extra
        k_pair[g * part:(g + 1) * part, :] = wide.T

    def step(t, c):
        jr = lax.rem(me + 1 + t, nodes)
        jl = lax.rem(me + nodes - t, nodes)
        hop(kv_all.at[jr], jr, t, to_left, from_right, left).wait_recv()

        @pl.when(t < half - 1)
        def _():
            hop(kv_all.at[jr], jr, t + 1, to_left, from_right, left).start()

        @pl.when(t > 0)
        def _():
            hop(kv_all.at[jl], jl, t - 1, to_right, from_left, right).wait_recv()

        @pl.when((t > 0) & (t < half - 1))
        def _():
            hop(kv_all.at[jl], jl, t, to_right, from_left, right).start()

        widen(jl, 0)
        widen(jr, 1)
        vl = kv_all[jl, head_dim:, :]
        vr = kv_all[jr, head_dim:, :]

        def body(h, c):
            lo = pl.multiple_of(h * LANES, LANES)
            r0 = pl.multiple_of(h * head_dim, head_dim)
            scores = dot(k_pair[...], q_wide[pl.ds(lo, LANES), :], 1, 0)
            old_max = max_ref[h]
            new_max = jnp.maximum(old_max, jnp.max(scores, axis=0, keepdims=True))
            prob = jnp.exp(scores - new_max)
            decay = jnp.exp(old_max - new_max)
            max_ref[h] = new_max
            sum_ref[h] = sum_ref[h] * decay + jnp.sum(prob, axis=0, keepdims=True)
            prob = prob.astype(BF16)
            acc_ref[pl.ds(r0, head_dim), :] = acc_ref[pl.ds(r0, head_dim), :] * decay + (dot(vl, prob[:part], 1, 0) + dot(vr, prob[part:], 1, 0))
            return c

        return lax.fori_loop(0, heads, body, c, unroll=unroll)

    lax.fori_loop(0, half, step, 0)

    def finish(h, c):
        r0 = pl.multiple_of(h * head_dim, head_dim)
        o_ref[pl.ds(r0, head_dim), :] = (acc_ref[pl.ds(r0, head_dim), :] / sum_ref[h]).astype(BF16)
        lse_ref[h] = max_ref[h] + jnp.log(sum_ref[h])
        return c

    lax.fori_loop(0, heads, finish, 0)

    def drain(t, c):
        hop(kv_ref, me, t, to_left, from_right, left).wait_send()

        @pl.when(t < half - 1)
        def _():
            hop(kv_ref, me, t, to_right, from_left, right).wait_send()
        return c

    lax.fori_loop(0, half, drain, 0)


def attention_forward(kv_t, key_bias, q_t, nodes, heads, head_dim, unroll=8):
    part = kv_t.shape[1]
    rows = q_t.shape[1]
    half = nodes // 2
    wide = jax.ShapeDtypeStruct((nodes, LANES, part), BF16)
    sems = lambda: pltpu.SemaphoreType.DMA((half,))
    return pl.pallas_call(
        functools.partial(forward_kernel, nodes=nodes, heads=heads, head_dim=head_dim, unroll=unroll),
        in_specs=[pl.BlockSpec(memory_space=pltpu.VMEM)] * 3,
        out_specs=[pl.BlockSpec(memory_space=pltpu.VMEM)] * 4,
        out_shape=[jax.ShapeDtypeStruct((heads * head_dim, rows), BF16), jax.ShapeDtypeStruct((heads, 1, rows), F32), wide, wide],
        scratch_shapes=[
            pltpu.VMEM((nodes, 2 * head_dim, part), BF16),
            pltpu.VMEM((2 * part, LANES), BF16),
            pltpu.VMEM((heads * LANES, rows), BF16),
            pltpu.VMEM((heads, 1, rows), F32),
            pltpu.VMEM((heads, 1, rows), F32),
            pltpu.VMEM((heads * head_dim, rows), F32),
            sems(), sems(), sems(), sems(),
        ],
        compiler_params=pltpu.CompilerParams(vmem_limit_bytes=40 * 2**20, collective_id=3, has_side_effects=True),
        cost_estimate=pl.CostEstimate(flops=4 * heads * rows * nodes * part * head_dim, bytes_accessed=2**23, transcendentals=heads * rows * nodes * part),
        name='attention_forward',
    )(kv_t, key_bias, q_t)


def backward_kernel(kt_ref, vt_ref, qt_ref, dot_ref, o_ref, lse_ref, dkv_ref, dq_ref, q_wide, do_wide, sums_r, sums_l, send_r, recv_r, send_l, recv_l, *, nodes, heads, head_dim, unroll):
    bk = kt_ref.shape[-1]
    me = lax.axis_index('nodes')
    right, left = lax.rem(me + 1, nodes), lax.rem(me + nodes - 1, nodes)
    barrier = pltpu.get_barrier_semaphore()
    for neighbour in (left, right):
        pl.semaphore_signal(barrier, inc=1, device_id={'nodes': neighbour}, device_id_type=MESH)
    dq_ref[...] = jnp.zeros_like(dq_ref)
    rows = qt_ref.shape[1]
    extra_iota = lax.broadcasted_iota(jnp.int32, (LANES - head_dim, rows), 0)

    def stack(parts):
        block = jnp.zeros((LANES - head_dim, rows), F32)
        for r, part in enumerate(parts):
            block = jnp.where(extra_iota == r, part, block)
        return block.astype(BF16)

    def split(x):
        hi = x.astype(BF16).astype(F32)
        mid = (x - hi).astype(BF16).astype(F32)
        return hi, mid, x - hi - mid

    def widen(h, c):
        r0 = pl.multiple_of(h * head_dim, head_dim)
        lo = pl.multiple_of(h * LANES, LANES)
        d_o = dot_ref[pl.ds(r0, head_dim), :]
        delta = jnp.sum(d_o.astype(F32) * o_ref[pl.ds(r0, head_dim), :].astype(F32), axis=0, keepdims=True)
        q_wide[:, pl.ds(lo, LANES)] = jnp.concatenate([qt_ref[pl.ds(r0, head_dim), :], stack((1.0,) + split(-lse_ref[h]))], axis=0).T
        do_wide[:, pl.ds(lo, LANES)] = jnp.concatenate([d_o, stack(split(-delta))], axis=0).T
        return c

    lax.fori_loop(0, heads, widen, 0)
    pl.semaphore_wait(barrier, 2)

    half = bk // 2
    rings = ((sums_r, send_r, recv_r, right, slice(0, half)), (sums_l, send_l, recv_l, left, slice(half, bk)))

    def hop(ring, t):
        sums, send_sem, recv_sem, to, cols = ring
        return pltpu.make_async_remote_copy(src_ref=sums.at[t], dst_ref=sums.at[t + 1], send_sem=send_sem.at[t], recv_sem=recv_sem.at[t + 1], device_id={'nodes': to}, device_id_type=MESH)

    def step(t, c):
        jr = lax.rem(me + 2 * nodes - 1 - t, nodes)
        jl = lax.rem(me + 1 + t, nodes)
        kt = jnp.concatenate([kt_ref[jr, :, :half], kt_ref[jl, :, half:]], axis=1)
        vt = jnp.concatenate([vt_ref[jr, :, :half], vt_ref[jl, :, half:]], axis=1)
        k_top = kt[:head_dim]

        def body(h, carry):
            dk, dv = carry
            lo = pl.multiple_of(h * LANES, LANES)
            r0 = pl.multiple_of(h * head_dim, head_dim)
            prob = jnp.exp(dot(q_wide[:, pl.ds(lo, LANES)], kt, 1, 0))
            d_prob = dot(do_wide[:, pl.ds(lo, LANES)], vt, 1, 0)
            d_scores = (prob * d_prob).astype(BF16)
            dv = dv + dot(dot_ref[pl.ds(r0, head_dim), :], prob.astype(BF16), 1, 0)
            dk = dk + dot(qt_ref[pl.ds(r0, head_dim), :], d_scores, 1, 0)
            dq_ref[pl.ds(r0, head_dim), :] += dot(k_top, d_scores, 1, 1)
            return dk, dv

        zero = jnp.zeros((head_dim, bk), F32)
        dk, dv = lax.fori_loop(0, heads, body, (zero, zero), unroll=unroll)

        @pl.when(t == 0)
        def _():
            for ring in rings:
                ring[0][t, :head_dim, :] = dk[:, ring[4]]
                ring[0][t, head_dim:, :] = dv[:, ring[4]]

        @pl.when(t > 0)
        def _():
            for ring in rings:
                hop(ring, t - 1).wait_recv()
                ring[0][t, :head_dim, :] += dk[:, ring[4]]
                ring[0][t, head_dim:, :] += dv[:, ring[4]]

        @pl.when(t < nodes - 1)
        def _():
            for ring in rings:
                hop(ring, t).start()
        return c

    lax.fori_loop(0, nodes, step, 0)

    def finish(t, c):
        for ring in rings:
            hop(ring, t).wait_send()
        return c

    lax.fori_loop(0, nodes - 1, finish, 0)
    for ring in rings:
        dkv_ref[:, ring[4]] = ring[0][nodes - 1].astype(BF16)


def attention_backward(kt_ext, vt_ext, q_t, do_t, mixed_t, log_norm, heads, head_dim, unroll=8):
    nodes, wide, bk = kt_ext.shape
    rows = q_t.shape[1]
    return pl.pallas_call(
        functools.partial(backward_kernel, nodes=nodes, heads=heads, head_dim=head_dim, unroll=unroll),
        in_specs=[pl.BlockSpec(memory_space=pltpu.VMEM)] * 6,
        out_specs=[pl.BlockSpec(memory_space=pltpu.VMEM)] * 2,
        out_shape=[jax.ShapeDtypeStruct((2 * head_dim, bk), BF16), jax.ShapeDtypeStruct((heads * head_dim, rows), F32)],
        scratch_shapes=[pltpu.VMEM((rows, heads * LANES), BF16)] * 2 + [pltpu.VMEM((nodes, 2 * head_dim, bk // 2), F32)] * 2 + [pltpu.SemaphoreType.DMA((nodes,))] * 4,
        compiler_params=pltpu.CompilerParams(vmem_limit_bytes=40 * 2**20, collective_id=0, has_side_effects=True),
        cost_estimate=pl.CostEstimate(flops=10 * heads * rows * nodes * bk * head_dim, bytes_accessed=2**24, transcendentals=heads * rows * nodes * bk),
        name='attention_backward',
    )(kt_ext, vt_ext, q_t, do_t, mixed_t, log_norm)


def exit_kernel(rows_ref, send_ix_ref, recv_ix_ref, x_ref, moved_ref, out_ref, send_buf, recv_buf, half, sums_r, sums_l, row_send, row_recv, pair_send, pair_recv, add_send_r, add_recv_r, add_send_l, add_recv_l, fill_send_r, fill_recv_r, fill_send_l, fill_recv_l, back_send_r, back_recv_r, back_send_l, back_recv_l, *, nodes):
    me = lax.axis_index('nodes')
    chips = nodes // 2
    core = lax.rem(me, 2)
    chip = me // 2
    partner = me + 1 - 2 * core
    hr = x_ref.shape[0] // 2
    pr = hr // chips
    mine = pl.multiple_of(core * hr, hr)
    other = pl.multiple_of((1 - core) * hr, hr)
    count, width = rows_ref.shape
    capacity = send_buf.shape[1]
    peer = lambda k: lax.rem(me + k, nodes)
    right = 2 * lax.rem(chip + 1, chips) + core
    left = 2 * lax.rem(chip + chips - 1, chips) + core
    barrier = pltpu.get_barrier_semaphore()

    def greet(k, c):
        pl.semaphore_signal(barrier, inc=1, device_id={'nodes': peer(k)}, device_id_type=MESH)
        return c

    lax.fori_loop(1, nodes, greet, 0)
    pl.semaphore_wait(barrier, nodes - 1)
    swap = pltpu.make_async_remote_copy(src_ref=x_ref.at[pl.ds(other, hr)], dst_ref=half, send_sem=pair_send, recv_sem=pair_recv, device_id={'nodes': partner}, device_id_type=MESH)
    swap.start()

    def give(k):
        return pltpu.make_async_remote_copy(src_ref=send_buf.at[k], dst_ref=recv_buf.at[me], send_sem=row_send.at[k], recv_sem=row_recv.at[k], device_id={'nodes': peer(k)}, device_id_type=MESH)

    cap_iota = lax.broadcasted_iota(jnp.int32, (capacity, count), 0)

    def pick_rows(k, c):
        pick = jnp.where(cap_iota + peer(k) * capacity == send_ix_ref[...], 1.0, 0.0).astype(BF16)
        send_buf[k] = dot(pick, rows_ref[...], 1, 0).astype(BF16)

        @pl.when(k > 0)
        def _():
            give(k).start()
        return c

    swap.wait_recv()
    half[...] += x_ref[pl.ds(mine, hr)]
    cut = sums_r.shape[2]
    rings = ((sums_r, 1, slice(0, cut), right, add_send_r, add_recv_r, fill_send_r, fill_recv_r, back_send_r, back_recv_r), (sums_l, chips - 1, slice(cut, x_ref.shape[1]), left, add_send_l, add_recv_l, fill_send_l, fill_recv_l, back_send_l, back_recv_l))

    def add_hop(ring, t):
        return pltpu.make_async_remote_copy(src_ref=ring[0].at[t], dst_ref=ring[0].at[t + 1], send_sem=ring[4].at[t], recv_sem=ring[5].at[t + 1], device_id={'nodes': ring[3]}, device_id_type=MESH)

    def add_step(t, c):
        for ring in rings:
            at = lax.rem(chip + (chips - ring[1]) * (t + 1), chips)
            term = half[pl.ds(pl.multiple_of(at * pr, pr), pr), ring[2]]

            @pl.when(t == 0)
            def _():
                ring[0][t] = term

            @pl.when(t > 0)
            def _():
                add_hop(ring, t - 1).wait_recv()
                ring[0][t] += term

            @pl.when(t < chips - 1)
            def _():
                add_hop(ring, t).start()

        return pick_rows(2 * t + 1, pick_rows(2 * t, c))

    lax.fori_loop(0, chips, add_step, 0)
    recv_buf[me] = send_buf[0]

    def place(t, ring):
        at = lax.rem(chip + (chips - ring[1]) * t, chips)
        return out_ref.at[pl.ds(pl.multiple_of(core * hr + at * pr, pr), pr), ring[2]]

    def fill_hop(ring, t):
        return pltpu.make_async_remote_copy(src_ref=place(t, ring), dst_ref=place(t, ring), send_sem=ring[6].at[t], recv_sem=ring[7].at[t + 1], device_id={'nodes': ring[3]}, device_id_type=MESH)

    def back_hop(ring, t):
        return pltpu.make_async_remote_copy(src_ref=place(t, ring), dst_ref=place(t, ring), send_sem=ring[8].at[t], recv_sem=ring[9].at[t], device_id={'nodes': partner}, device_id_type=MESH)

    for ring in rings:
        out_ref[pl.ds(pl.multiple_of(core * hr + chip * pr, pr), pr), ring[2]] = ring[0][chips - 1]

    def fill_step(t, c):
        for ring in rings:
            @pl.when(t > 0)
            def _():
                fill_hop(ring, t - 1).wait_recv()

            @pl.when(t < chips - 1)
            def _():
                fill_hop(ring, t).start()

            back_hop(ring, t).start()
        return c

    lax.fori_loop(0, chips, fill_step, 0)

    def wait_rows(k, c):
        give(k).wait_recv()
        return c

    lax.fori_loop(1, nodes, wait_rows, 0)
    landed = jnp.where(lax.broadcasted_iota(jnp.int32, (nodes * capacity, count), 0) == recv_ix_ref[...], 1.0, 0.0).astype(BF16)
    moved_ref[...] = dot(landed, recv_buf[...].reshape(nodes * capacity, width), 0, 0).astype(BF16)

    def wait_sends(k, c):
        give(k).wait_send()
        return c

    lax.fori_loop(1, nodes, wait_sends, 0)
    swap.wait_send()

    def drain(t, c):
        for ring in rings:
            back_hop(ring, t).wait()

            @pl.when(t < chips - 1)
            def _():
                add_hop(ring, t).wait_send()
                fill_hop(ring, t).wait_send()
        return c

    lax.fori_loop(0, chips, drain, 0)


def exit_moves(rows, send_ix, recv_ix, x, nodes):
    count, width = rows.shape
    total, cols = x.shape
    chips = nodes // 2
    pr = total // nodes
    cut = (cols // LANES + 1) // 2 * LANES
    capacity = count // nodes + count // (2 * nodes)
    row_sems = [pltpu.SemaphoreType.DMA((nodes,))] * 2
    return pl.pallas_call(
        functools.partial(exit_kernel, nodes=nodes),
        in_specs=[pl.BlockSpec(memory_space=pltpu.VMEM)] * 4,
        out_specs=[pl.BlockSpec(memory_space=pltpu.VMEM)] * 2,
        out_shape=[jax.ShapeDtypeStruct(rows.shape, BF16), jax.ShapeDtypeStruct(x.shape, F32)],
        scratch_shapes=[pltpu.VMEM((nodes, capacity, width), BF16)] * 2
        + [pltpu.VMEM((total // 2, cols), F32), pltpu.VMEM((chips, pr, cut), F32), pltpu.VMEM((chips, pr, cols - cut), F32)]
        + row_sems + [pltpu.SemaphoreType.DMA] * 2 + [pltpu.SemaphoreType.DMA((chips,))] * 12,
        compiler_params=pltpu.CompilerParams(vmem_limit_bytes=24 * 2**20, collective_id=1, has_side_effects=True),
        cost_estimate=pl.CostEstimate(flops=10**10, bytes_accessed=2**23, transcendentals=0),
        name='exit_moves',
    )(rows, send_ix.reshape(1, -1), recv_ix.reshape(1, -1), x)


def one_hot(index, size):
    return (lax.broadcasted_iota(jnp.int32, (size, index.size), 0) == index[None, :]).astype(BF16)


def exchange(rows, send_ix, recv_ix, nodes, after=()):
    count, width = rows.shape
    capacity = count // nodes + count // (2 * nodes)
    picked = dot(one_hot(send_ix, nodes * capacity), rows, 1, 0).astype(BF16)
    picked, after = lax.optimization_barrier((picked, after))
    landed = lax.all_to_all(picked.reshape(nodes, capacity, width), 'nodes', 0, 0, tiled=True)
    return dot(one_hot(recv_ix, nodes * capacity), landed.reshape(nodes * capacity, width), 0, 0).astype(BF16), after


def solution(mesh):
    nodes = mesh.shape['nodes']
    row_spec = P(('graphs', 'nodes'), None)
    flat_spec = P(('graphs', 'nodes'))
    halo_spec = P(('graphs', 'nodes'), None, None)
    grad_spec = P('graphs', None)

    def device_step(x_feat, valid, halo_slot, edge_src, edge_dst, edge_mask, bal_perm, pos_enc, y_cot, w_msg, w_self, w_q, w_k, w_v, w_o, w_up, w_down):
        rows_dev, width = x_feat.shape
        head_dim = w_k.shape[1]
        heads = width // head_dim
        scale = head_dim ** -0.5
        halo_rows = halo_slot.size

        count = jnp.sum((valid > 0).astype(jnp.int32))
        info = jnp.concatenate([bal_perm, jnp.broadcast_to(count, (LANES,))])[None, None, :]
        halo_ask = jnp.pad(halo_slot.reshape(nodes, 1, -1), ((0, 0), (0, 0), (0, LANES - halo_rows // nodes)))
        live_dst = jnp.where(edge_mask.reshape(-1) > 0, edge_dst.reshape(-1), -1)
        x_bal, adjacency, bal_ix, part_ix, info_all, halo_got, halo_feat = entry(x_feat, info, halo_ask, halo_rows // nodes, edge_src.reshape(-1), live_dst, nodes)
        bal_ix, part_ix = bal_ix.reshape(-1), part_ix.reshape(-1)
        bal_all = info_all[:, 0, :rows_dev]
        owner_all = bal_all // rows_dev
        limit = jnp.sum(jnp.where(owner_all[:, :, None] == jnp.arange(nodes, dtype=jnp.int32), info_all[None, None, :, 0, rows_dev], 0), axis=2)
        key_bias = jnp.where(bal_all % rows_dev < limit, 0.0, NEG_FILL)[:, None, :]

        hidden_in = (x_bal.astype(F32) + pos_enc.astype(F32)).astype(BF16)
        w_kv = jnp.concatenate([w_k, w_v], axis=1)
        kv_t = dot(w_kv, hidden_in, 0, 1).astype(BF16)
        q_t = dot((w_q.astype(F32) * scale).astype(BF16), hidden_in, 0, 1).astype(BF16)

        halo_got = halo_got[:, 0, :halo_rows // nodes].reshape(-1)
        halo_pick = one_hot(halo_got, rows_dev)
        halo_feat = halo_feat.reshape(halo_rows, width)
        adj_own, adj_halo = adjacency[:, :rows_dev], adjacency[:, rows_dev:]
        agg_msg = (dot(adj_own, x_feat, 1, 0) + dot(adj_halo, halo_feat, 1, 0)).astype(BF16)
        pre_act = dot(agg_msg, w_msg, 1, 0) + dot(x_feat, w_self, 1, 0)

        mixed_t, log_norm, kt_ext, vt_ext = attention_forward(kv_t, key_bias, q_t, nodes, heads, head_dim)
        u_bal = dot(mixed_t, w_o, 0, 0).astype(BF16)
        u_part, unused = exchange(u_bal, bal_ix, part_ix, nodes)

        x_wide = x_feat.astype(F32)
        z_mid = (x_wide + jax.nn.relu(pre_act) + x_wide + u_part.astype(F32)).astype(BF16)
        h_pre = dot(z_mid, w_up, 1, 0)
        hidden = jax.nn.gelu(h_pre).astype(BF16)
        keep_row = valid[:, None] > 0
        y_out = jnp.where(keep_row, z_mid.astype(F32) + dot(hidden, w_down, 1, 0), 0.0).astype(BF16)

        g_out = jnp.where(keep_row, y_cot, jnp.zeros_like(y_cot))
        d_hidden = dot(g_out, w_down, 1, 1).astype(BF16)
        gelu_pull = jax.vjp(jax.nn.gelu, h_pre)[1]
        d_hpre = gelu_pull(d_hidden.astype(F32))[0].astype(BF16)
        d_z = (g_out.astype(F32) + dot(d_hpre, w_up, 1, 1)).astype(BF16)
        d_u, (g_late, d_hlate) = exchange(d_z, part_ix, bal_ix, nodes, (g_out, d_hpre))

        grad_down = dot(hidden, g_late, 0, 0)
        grad_up = dot(z_mid, d_hlate, 0, 0)
        d_pre = jnp.where(pre_act > 0, d_z, jnp.zeros_like(d_z))
        grad_self = dot(x_feat, d_pre, 0, 0)
        grad_msg = dot(agg_msg, d_pre, 0, 0)
        grad_msg, grad_self, grad_up, grad_down = lax.psum((grad_msg, grad_self, grad_up, grad_down), 'nodes')

        do_t = dot(w_o, d_u, 1, 1).astype(BF16)
        grad_o = dot(mixed_t, d_u, 1, 0)
        dkv_t, dq_t = attention_backward(kt_ext, vt_ext, q_t, do_t, mixed_t, log_norm, heads, head_dim)
        dq_t = (dq_t * scale).astype(BF16)

        d_agg = dot(d_pre, w_msg, 1, 1).astype(BF16)
        d_halo = dot(adj_halo, d_agg, 0, 0).astype(BF16)
        halo_landed = lax.all_to_all(d_halo.reshape(nodes, -1, width), 'nodes', 0, 0, tiled=True).reshape(halo_rows, width)
        local_part = 2.0 * d_z.astype(F32) + dot(d_pre, w_self, 1, 1) + dot(adj_own, d_agg, 0, 0) + dot(halo_pick, halo_landed, 1, 0)

        grad_q = dot(hidden_in, dq_t, 0, 1)
        grad_kv = dot(hidden_in, dkv_t, 0, 1)
        dx_bal = dot(jnp.concatenate([dq_t, dkv_t], axis=0), jnp.concatenate([w_q, w_kv], axis=1), 0, 1).astype(BF16)
        attn_back, late = exit_moves(dx_bal, bal_ix, part_ix, jnp.concatenate([grad_q, grad_o, grad_kv], axis=1), nodes)
        dx_feat = (local_part + attn_back.astype(F32)).astype(BF16)
        grad_q, grad_o, grad_k, grad_v = late[:, :width], late[:, width:2 * width], late[:, 2 * width:2 * width + head_dim], late[:, 2 * width + head_dim:]
        return y_out, dx_feat, grad_msg, grad_self, grad_q, grad_k, grad_v, grad_o, grad_up, grad_down

    return jax.shard_map(device_step, mesh=mesh, in_specs=(row_spec, flat_spec, halo_spec, row_spec, row_spec, row_spec, flat_spec, row_spec, row_spec) + (P(),) * 8, out_specs=(row_spec, row_spec) + (grad_spec,) * 8, check_vma=False)
```
